32 devices in a mesh: dp: 32 (over z, y, x, core).
Axes of the slice: x: 2, y: 2, z: 4, core: 2. Of those that a mesh axis runs over, the one named last changes fastest.
Arguments:
- x_saved: bfloat16 [192, 256, 896], P('dp')
- grad_out: bfloat16 [192, 256, 896], P('dp')
- positions: int32 [192, 256], P('dp')
- attn_gain: bfloat16 [896], replicated
- w_query: bfloat16 [896, 14, 64], replicated
- w_key: bfloat16 [896, 2, 64], replicated
- w_value: bfloat16 [896, 2, 64], replicated
- w_out: bfloat16 [14, 64, 896], replicated
- mlp_gain: bfloat16 [896], replicated
- w_gate: bfloat16 [896, 4864], replicated
- w_up: bfloat16 [896, 4864], replicated
- w_down: bfloat16 [4864, 896], replicated
- master_flat: float32 [14911232], P('dp')
- adam_mean: float32 [14911232], P('dp')
- adam_var: float32 [14911232], P('dp')
Outputs:
- output 1: bfloat16 [192, 256, 896], P('dp')
- output 2: bfloat16 [896], replicated
- output 3: bfloat16 [896, 14, 64], replicated
- output 4: bfloat16 [896, 2, 64], replicated
- output 5: bfloat16 [896, 2, 64], replicated
- output 6: bfloat16 [14, 64, 896], replicated
- output 7: bfloat16 [896], replicated
- output 8: bfloat16 [896, 4864], replicated
- output 9: bfloat16 [896, 4864], replicated
- output 10: bfloat16 [4864, 896], replicated
- output 11: float32 [14911232], P('dp')
- output 12: float32 [14911232], P('dp')
- output 13: float32 [14911232], P('dp')
- output 14: float32 [], replicated
All inputs are finite; a program needn't handle non-finite values.
Results may differ from the reference program's by a relative error of at most 0.0147953.
Values are sent between devices in bfloat16 or wider.
A program may use at most 1 GiB of HBM per device.

```python
import math
import jax
import jax.numpy as jnp
from jax import lax

MODEL_DIM = 896
NUM_HEADS = 14
KV_HEADS = 2
HEAD_DIM = 64
FFN_DIM = 4864
SEQ_LEN = 256
SEQS_DEV = 6
DP_SIZE = 32
STEP_COUNT = 100
TOTAL_SEQS = SEQS_DEV * DP_SIZE
NPARAM = MODEL_DIM * (2 + 2 * HEAD_DIM * (NUM_HEADS + KV_HEADS) + 3 * FFN_DIM)
NORM_EPS = 1e-5
ROPE_BASE = 10000.0
LEARN_RATE = 2e-3
BETA_ONE = 0.9
BETA_TWO = 0.95
ADAM_EPS = 1e-8
WEIGHT_DECAY = 0.1


def param_shapes():
    return [(MODEL_DIM,), (MODEL_DIM, NUM_HEADS, HEAD_DIM), (MODEL_DIM, KV_HEADS, HEAD_DIM),
            (MODEL_DIM, KV_HEADS, HEAD_DIM), (NUM_HEADS, HEAD_DIM, MODEL_DIM), (MODEL_DIM,),
            (MODEL_DIM, FFN_DIM), (MODEL_DIM, FFN_DIM), (FFN_DIM, MODEL_DIM)]


def draw_params(key):
    key_list = jax.random.split(key, 9)
    fan_ins = [0, MODEL_DIM, MODEL_DIM, MODEL_DIM, NUM_HEADS * HEAD_DIM, 0, MODEL_DIM, MODEL_DIM, FFN_DIM]
    drawn_list = []
    for number, piece_shape in enumerate(param_shapes()):
        noise_arr = jax.random.normal(key_list[number], piece_shape, jnp.float32)
        if fan_ins[number] == 0:
            drawn_list.append(1.0 + 0.2 * noise_arr)
        else:
            drawn_list.append(noise_arr * fan_ins[number] ** -0.5)
    return drawn_list


def setup_inputs(seed: int = 0) -> dict:
    key_list = jax.random.split(jax.random.key(seed), 8)
    act_shape = (TOTAL_SEQS, SEQ_LEN, MODEL_DIM)
    x_saved = jax.random.normal(key_list[0], act_shape, jnp.float32).astype(jnp.bfloat16)
    grad_out = jax.random.normal(key_list[1], act_shape, jnp.float32).astype(jnp.bfloat16)
    pos_gaps = jax.random.randint(key_list[2], (TOTAL_SEQS, SEQ_LEN), 1, 4)
    positions = (jnp.cumsum(pos_gaps, axis=1) - 1).astype(jnp.int32)
    weights = [w_piece.astype(jnp.bfloat16) for w_piece in draw_params(key_list[3])]
    master_flat = jnp.concatenate([w_piece.reshape(-1) for w_piece in draw_params(key_list[4])])
    state_scale = NPARAM ** -0.5
    adam_mean = 0.1 * state_scale * jax.random.normal(key_list[5], (NPARAM,), jnp.float32)
    var_root = 0.3 * state_scale * jax.random.uniform(key_list[6], (NPARAM,), jnp.float32, 0.5, 1.5)
    adam_var = var_root * var_root
    return {'x_saved': x_saved, 'grad_out': grad_out, 'positions': positions,
            'attn_gain': weights[0], 'w_query': weights[1], 'w_key': weights[2], 'w_value': weights[3],
            'w_out': weights[4], 'mlp_gain': weights[5], 'w_gate': weights[6], 'w_up': weights[7],
            'w_down': weights[8], 'master_flat': master_flat, 'adam_mean': adam_mean, 'adam_var': adam_var}


def rms_scale(values, gain):
    wide = values.astype(jnp.float32)
    inv_rms = lax.rsqrt(jnp.mean(wide * wide, axis=-1, keepdims=True) + NORM_EPS)
    return (wide * inv_rms * gain.astype(jnp.float32)).astype(jnp.bfloat16)


def rope_tables(positions, head_dim):
    half_dim = head_dim // 2
    inv_freq = ROPE_BASE ** (-2.0 * jnp.arange(half_dim, dtype=jnp.float32) / head_dim)
    angles = positions.astype(jnp.float32)[:, :, None] * inv_freq
    cos_full = jnp.concatenate([jnp.cos(angles), jnp.cos(angles)], axis=-1)[:, :, None, :]
    sin_full = jnp.concatenate([jnp.sin(angles), jnp.sin(angles)], axis=-1)[:, :, None, :]
    return cos_full, sin_full


def rope_apply(values, cos_full, sin_full):
    half_dim = values.shape[-1] // 2
    rotated = jnp.concatenate([-values[..., half_dim:], values[..., :half_dim]], axis=-1)
    return values * cos_full + rotated * sin_full


def layer_forward(w_list, x_val, positions):
    attn_gain, w_query, w_key, w_value, w_out, mlp_gain, w_gate, w_up, w_down = w_list
    num_seqs, seq_len, model_dim = x_val.shape
    num_heads, head_dim = w_query.shape[1], w_query.shape[2]
    kv_heads = w_key.shape[1]
    group_size = num_heads // kv_heads
    n_tok = num_seqs * seq_len
    x_flat = x_val.reshape(n_tok, model_dim)
    normed = rms_scale(x_flat, attn_gain)
    q_pre = jnp.dot(normed, w_query.reshape(model_dim, num_heads * head_dim), preferred_element_type=jnp.float32)
    k_pre = jnp.dot(normed, w_key.reshape(model_dim, kv_heads * head_dim), preferred_element_type=jnp.float32)
    v_pre = jnp.dot(normed, w_value.reshape(model_dim, kv_heads * head_dim), preferred_element_type=jnp.float32)
    v_heads = v_pre.astype(jnp.bfloat16).reshape(num_seqs, seq_len, kv_heads, head_dim)
    cos_full, sin_full = rope_tables(positions, head_dim)
    q_rot = rope_apply(q_pre.reshape(num_seqs, seq_len, num_heads, head_dim), cos_full, sin_full).astype(jnp.bfloat16)
    q_rot = q_rot.reshape(num_seqs, seq_len, kv_heads, group_size, head_dim)
    k_rot = rope_apply(k_pre.reshape(num_seqs, seq_len, kv_heads, head_dim), cos_full, sin_full).astype(jnp.bfloat16)
    scores = jnp.einsum('bqkgd,bskd->bkgqs', q_rot.astype(jnp.float32), k_rot.astype(jnp.float32)) * head_dim ** -0.5
    causal = jnp.arange(seq_len)[:, None] >= jnp.arange(seq_len)[None, :]
    attn_probs = jax.nn.softmax(jnp.where(causal, scores, -1e30), axis=-1).astype(jnp.bfloat16)
    context = jnp.einsum('bkgqs,bskd->bqkgd', attn_probs.astype(jnp.float32), v_heads.astype(jnp.float32)).astype(jnp.bfloat16)
    attn_out = jnp.dot(context.reshape(n_tok, num_heads * head_dim), w_out.reshape(num_heads * head_dim, model_dim), preferred_element_type=jnp.float32)
    hidden = (x_flat.astype(jnp.float32) + attn_out).astype(jnp.bfloat16)
    normed_mlp = rms_scale(hidden, mlp_gain)
    gate_pre = jnp.dot(normed_mlp, w_gate, preferred_element_type=jnp.float32)
    up_pre = jnp.dot(normed_mlp, w_up, preferred_element_type=jnp.float32)
    gated_act = (jax.nn.silu(gate_pre) * up_pre).astype(jnp.bfloat16)
    down_out = jnp.dot(gated_act, w_down, preferred_element_type=jnp.float32)
    return (hidden.astype(jnp.float32) + down_out).astype(jnp.bfloat16).reshape(num_seqs, seq_len, model_dim)


def split_flat(flat_vec):
    pieces = []
    offset = 0
    for piece_shape in param_shapes():
        piece_size = math.prod(piece_shape)
        pieces.append(flat_vec[offset:offset + piece_size].reshape(piece_shape))
        offset += piece_size
    return pieces


def reference(x_saved, grad_out, positions, attn_gain, w_query, w_key, w_value, w_out, mlp_gain, w_gate, w_up, w_down, master_flat, adam_mean, adam_var):
    w_list = (attn_gain, w_query, w_key, w_value, w_out, mlp_gain, w_gate, w_up, w_down)

    def device_grads(grad_acc, group_in):
        x_group, dy_group, pos_group = group_in
        layer_out, pullback = jax.vjp(lambda x_val, w_vals: layer_forward(w_vals, x_val, pos_group), x_group, w_list)
        grad_x, grad_w = pullback(dy_group)
        flat_grad = jnp.concatenate([w_grad.astype(jnp.bfloat16).reshape(-1).astype(jnp.float32) for w_grad in grad_w])
        return grad_acc + flat_grad, grad_x.astype(jnp.bfloat16)

    group_shape = (DP_SIZE, SEQS_DEV, SEQ_LEN, MODEL_DIM)
    grad_sum, grad_x = lax.scan(device_grads, jnp.zeros((NPARAM,), jnp.float32),
                                (x_saved.reshape(group_shape), grad_out.reshape(group_shape),
                                 positions.reshape(DP_SIZE, SEQS_DEV, SEQ_LEN)))
    grad_mean = grad_sum / DP_SIZE
    grad_norm = jnp.sqrt(jnp.sum(grad_mean * grad_mean))
    clip_scale = jnp.minimum(1.0, 1.0 / (grad_norm + 1e-6))
    clipped = grad_mean * clip_scale
    new_mean = BETA_ONE * adam_mean + (1.0 - BETA_ONE) * clipped
    new_var = BETA_TWO * adam_var + (1.0 - BETA_TWO) * clipped * clipped
    mean_hat = new_mean / (1.0 - BETA_ONE ** STEP_COUNT)
    var_hat = new_var / (1.0 - BETA_TWO ** STEP_COUNT)
    gain_two = MODEL_DIM + 2 * MODEL_DIM * HEAD_DIM * (NUM_HEADS + KV_HEADS)
    flat_index = jnp.arange(NPARAM)
    is_gain = (flat_index < MODEL_DIM) | ((flat_index >= gain_two) & (flat_index < gain_two + MODEL_DIM))
    decays = jnp.where(is_gain, 0.0, WEIGHT_DECAY)
    new_master = master_flat - LEARN_RATE * (mean_hat / (jnp.sqrt(var_hat) + ADAM_EPS) + decays * master_flat)
    new_weights = split_flat(new_master.astype(jnp.bfloat16))
    return (grad_x.reshape(TOTAL_SEQS, SEQ_LEN, MODEL_DIM), new_weights[0], new_weights[1], new_weights[2],
            new_weights[3], new_weights[4], new_weights[5], new_weights[6], new_weights[7], new_weights[8],
            new_master, new_mean, new_var, grad_norm)
```

```python
import jax
import jax.numpy as jnp
from jax import lax
from jax.experimental import pallas as pl
from jax.experimental.pallas import tpu as pltpu
from jax.sharding import PartitionSpec as P

NORM_EPS = 1e-5
ROPE_BASE = 10000.0
LEARN_RATE = 2e-3
BETA_ONE = 0.9
BETA_TWO = 0.95
ADAM_EPS = 1e-8
WEIGHT_DECAY = 0.1
STEP_COUNT = 100


DEVS = 32
UNIT = 1024
BLOCK = 465976
ATT_UNITS = 56
MLP_UNITS = 133
GAIN_UNIT = 1 + DEVS * ATT_UNITS
MLP_UNIT = GAIN_UNIT + 1
GAIN_TWO = 1835904
CHUNK = 7
HALO = 8192
HALO_UNITS = HALO // UNIT
CORE_UNITS = 457
WINDOW = CORE_UNITS + 17
SHARD = ATT_UNITS + 1 + 3 * MLP_UNITS
PIECES = ((0, 1, ATT_UNITS), (ATT_UNITS + 1, MLP_UNIT, MLP_UNITS),
          (ATT_UNITS + 1 + MLP_UNITS, MLP_UNIT + DEVS * MLP_UNITS, MLP_UNITS),
          (ATT_UNITS + 1 + 2 * MLP_UNITS, MLP_UNIT + 2 * DEVS * MLP_UNITS, MLP_UNITS))


def as_units(grad):
    return grad.astype(jnp.bfloat16).reshape(-1, 8, 128)


def scatter(units):
    return lax.psum_scatter(units, 'dp', scatter_dimension=0, tiled=True)


def first_unit(owner):
    return (BLOCK * owner + 128) // UNIT


def last_owner(unit):
    return jnp.minimum((UNIT * (unit + CHUNK) - 129) // BLOCK, DEVS - 1)


def first_owner(unit):
    return (jnp.maximum(UNIT * (unit - CORE_UNITS + 1) - 128, 0) + BLOCK - 1) // BLOCK


def start_copy(source, target, peer, me, send_sem, recv_sem):
    @pl.when(peer == me)
    def _():
        pltpu.make_async_copy(source, target, recv_sem).start()

    @pl.when(peer != me)
    def _():
        pltpu.make_async_remote_copy(source, target, send_sem, recv_sem, device_id={'dp': peer}).start()


def end_send(source, target, peer, me, send_sem, recv_sem):
    @pl.when(peer != me)
    def _():
        pltpu.make_async_remote_copy(source, target, send_sem, recv_sem, device_id={'dp': peer}).wait_send()


def end_recv(source, target, recv_sem):
    pltpu.make_async_copy(source, target, recv_sem).wait()


def reach(unit, base, total):
    return jnp.minimum(jnp.maximum(unit - base, 0) // CHUNK, total)


def owned_chunks(owner, action):
    for base, total in ((1, DEVS * ATT_UNITS // CHUNK), (MLP_UNIT, 3 * DEVS * MLP_UNITS // CHUNK)):
        def step(index, carry, base=base):
            action(base + index * CHUNK)
            return carry
        low = first_unit(owner)
        lax.fori_loop(reach(low, base, total), reach(low + CORE_UNITS + CHUNK - 1, base, total), step, 0)


def window_slot(unit, owner):
    return unit - first_unit(owner) + HALO_UNITS


def spread_kernel(shard_ref, part_ref, window_ref, parts_ref, send_sems, recv_sems, part_send, part_recv, gain_send, gain_recv):
    me = lax.axis_index('dp')
    gain_owner = GAIN_TWO // BLOCK

    def place(unit, owner, size=CHUNK):
        return window_ref.at[pl.ds(window_slot(unit, owner), size)]

    def part_copy(step):
        return pltpu.make_async_remote_copy(part_ref, parts_ref.at[pl.ds(me, 1)], part_send.at[step], part_recv.at[me],
                                            device_id={'dp': lax.rem(me + step, DEVS)})

    def start_part(step, carry):
        part_copy(step).start()
        return carry

    def end_part(step, carry):
        part_copy(step).wait_send()
        return carry

    def take_part(peer, carry):
        end_recv(part_ref, parts_ref.at[pl.ds(peer, 1)], part_recv.at[peer])
        return carry

    def each_chunk(action):
        first = 0
        for offset, base, count in PIECES:
            def step(index, carry, offset=offset, base=base, count=count, first=first):
                source = shard_ref.at[pl.ds(offset + index * CHUNK, CHUNK)]
                unit = base + me * count + index * CHUNK
                low, high = first_owner(unit), last_owner(unit)
                action(source, place(unit, high), high, me, send_sems.at[2 * (first + index)], recv_sems.at[window_slot(unit, high) // CHUNK])

                @pl.when(low != high)
                def _():
                    action(source, place(unit, low), low, me, send_sems.at[2 * (first + index) + 1],
                           recv_sems.at[window_slot(unit, low) // CHUNK])
                return carry
            lax.fori_loop(0, count // CHUNK, step, 0)
            first += count // CHUNK

    gain_source = shard_ref.at[pl.ds(ATT_UNITS, 1)]
    gain_two = pltpu.make_async_remote_copy(gain_source, place(GAIN_UNIT, gain_owner, 1), gain_send, gain_recv, device_id={'dp': gain_owner})
    gain_one = pltpu.make_async_copy(gain_source, place(0, 0, 1), gain_recv)
    pltpu.make_async_copy(part_ref, parts_ref.at[pl.ds(me, 1)], part_recv.at[me]).start()
    lax.fori_loop(1, DEVS, start_part, 0)

    @pl.when(me == 0)
    def _():
        gain_one.start()

    @pl.when(me == 1)
    def _():
        gain_two.start()

    each_chunk(start_copy)
    owned_chunks(me, lambda unit: end_recv(shard_ref.at[pl.ds(0, CHUNK)], place(unit, me), recv_sems.at[window_slot(unit, me) // CHUNK]))
    each_chunk(end_send)
    lax.fori_loop(0, DEVS, take_part, 0)
    lax.fori_loop(1, DEVS, end_part, 0)

    @pl.when(me == 0)
    def _():
        gain_one.wait()

    @pl.when(me == 1)
    def _():
        gain_two.wait_send()

    @pl.when(me == gain_owner)
    def _():
        pltpu.make_async_copy(gain_source, place(GAIN_UNIT, me, 1), gain_recv).wait()


def collect_kernel(window_ref, shard_ref, send_sems, recv_sems, gain_send, gain_recv):
    me = lax.axis_index('dp')
    gain_owner = GAIN_TWO // BLOCK

    def slot(unit, size=CHUNK):
        return window_ref.at[pl.ds(window_slot(unit, me), size)]

    def each_chunk(action):
        first = 0
        for offset, base, count in PIECES:
            per = count // CHUNK
            total = DEVS * per

            def step(index, carry, offset=offset, base=base, per=per, first=first):
                peer = index // per
                within = index - peer * per
                unit = base + index * CHUNK
                action(slot(unit), shard_ref.at[pl.ds(offset + within * CHUNK, CHUNK)], peer, me,
                       send_sems.at[window_slot(unit, me) // CHUNK], recv_sems.at[first + within])
                return carry
            low = reach(first_unit(me), base, total)
            high = jnp.where(me == DEVS - 1, total, reach(first_unit(me + 1), base, total))
            lax.fori_loop(low, high, step, 0)
            first += per

    def take(index, carry):
        end_recv(window_ref.at[pl.ds(0, CHUNK)], shard_ref.at[pl.ds(0, CHUNK)], recv_sems.at[index])
        return carry

    gain_target = shard_ref.at[pl.ds(ATT_UNITS, 1)]
    gain_two = pltpu.make_async_remote_copy(slot(GAIN_UNIT, 1), gain_target, gain_send, gain_recv, device_id={'dp': 1})
    gain_one = pltpu.make_async_copy(slot(0, 1), gain_target, gain_recv)

    @pl.when(me == 0)
    def _():
        gain_one.start()

    @pl.when(me == gain_owner)
    def _():
        gain_two.start()

    each_chunk(start_copy)
    lax.fori_loop(0, (SHARD - 1) // CHUNK, take, 0)
    each_chunk(end_send)

    @pl.when(me == 0)
    def _():
        gain_one.wait()

    @pl.when(me == gain_owner)
    def _():
        gain_two.wait_send()

    @pl.when(me == 1)
    def _():
        pltpu.make_async_copy(window_ref.at[pl.ds(0, 1)], gain_target, gain_recv).wait()


VMEM = pl.BlockSpec(memory_space=pltpu.VMEM)


def spread(shard, part):
    return pl.pallas_call(
        spread_kernel,
        out_shape=(jax.ShapeDtypeStruct((WINDOW, 8, 128), jnp.bfloat16), jax.ShapeDtypeStruct((DEVS, 8, 128), jnp.float32)),
        in_specs=[VMEM, VMEM], out_specs=(VMEM, VMEM),
        scratch_shapes=[pltpu.SemaphoreType.DMA((2 * (SHARD - 1) // CHUNK,)), pltpu.SemaphoreType.DMA((WINDOW // CHUNK + 1,)),
                        pltpu.SemaphoreType.DMA((DEVS,)), pltpu.SemaphoreType.DMA((DEVS,)), pltpu.SemaphoreType.DMA, pltpu.SemaphoreType.DMA],
        compiler_params=pltpu.CompilerParams(has_side_effects=True),
    )(shard, part)


def collect(window):
    return pl.pallas_call(
        collect_kernel,
        out_shape=jax.ShapeDtypeStruct((SHARD, 8, 128), jnp.bfloat16),
        in_specs=[VMEM], out_specs=VMEM,
        scratch_shapes=[pltpu.SemaphoreType.DMA((WINDOW // CHUNK + 1,)), pltpu.SemaphoreType.DMA(((SHARD - 1) // CHUNK,)),
                        pltpu.SemaphoreType.DMA, pltpu.SemaphoreType.DMA],
        compiler_params=pltpu.CompilerParams(has_side_effects=True),
    )(window)


def rope_tables(positions, head_dim):
    half_dim = head_dim // 2
    inv_freq = ROPE_BASE ** (-2.0 * jnp.arange(half_dim, dtype=jnp.float32) / head_dim)
    angles = positions.astype(jnp.float32)[:, :, None] * inv_freq
    cos_full = jnp.concatenate([jnp.cos(angles), jnp.cos(angles)], axis=-1)[:, :, None, :]
    sin_full = jnp.concatenate([jnp.sin(angles), jnp.sin(angles)], axis=-1)[:, :, None, :]
    return cos_full, sin_full


def rope_apply(values, cos_full, sin_full):
    half_dim = values.shape[-1] // 2
    rotated = jnp.concatenate([-values[..., half_dim:], values[..., :half_dim]], axis=-1)
    return values * cos_full + rotated * sin_full


def rope_back(grad_rot, cos_full, sin_full):
    half_dim = grad_rot.shape[-1] // 2
    scaled = grad_rot * sin_full
    return grad_rot * cos_full + jnp.concatenate([scaled[..., half_dim:], -scaled[..., :half_dim]], axis=-1)


def rms_parts(values):
    inv_rms = lax.rsqrt(jnp.mean(values * values, axis=-1, keepdims=True) + NORM_EPS)
    return inv_rms, values * inv_rms


def rms_back(d_normed, gain_wide, inv_rms, x_hat):
    d_hat = d_normed * gain_wide
    return inv_rms * (d_hat - x_hat * jnp.mean(d_hat * x_hat, axis=-1, keepdims=True))


def local_grads(x_loc, dy_loc, pos_loc, w_list, halos):
    attn_gain, w_query, w_key, w_value, w_out, mlp_gain, w_gate, w_up, w_down = w_list
    num_seqs, seq_len, model_dim = x_loc.shape
    num_heads, head_dim = w_query.shape[1], w_query.shape[2]
    kv_heads = w_key.shape[1]
    group_size = num_heads // kv_heads
    n_tok = num_seqs * seq_len
    wq_flat = w_query.reshape(model_dim, num_heads * head_dim)
    wk_flat = w_key.reshape(model_dim, kv_heads * head_dim)
    wv_flat = w_value.reshape(model_dim, kv_heads * head_dim)
    wo_flat = w_out.reshape(num_heads * head_dim, model_dim)
    dy_flat = dy_loc.reshape(n_tok, model_dim)
    x_wide = x_loc.reshape(n_tok, model_dim).astype(jnp.float32)
    inv_one, value_a8 = rms_parts(x_wide)
    gain_one = attn_gain.astype(jnp.float32)
    normed = (value_a8 * gain_one).astype(jnp.bfloat16)
    q_pre = jnp.dot(normed, wq_flat, preferred_element_type=jnp.float32).reshape(num_seqs, seq_len, num_heads, head_dim)
    k_pre = jnp.dot(normed, wk_flat, preferred_element_type=jnp.float32).reshape(num_seqs, seq_len, kv_heads, head_dim)
    v_heads = jnp.dot(normed, wv_flat, preferred_element_type=jnp.float32).astype(jnp.bfloat16).reshape(num_seqs, seq_len, kv_heads, head_dim)
    cos_full, sin_full = rope_tables(pos_loc, head_dim)
    q_rot = rope_apply(q_pre, cos_full, sin_full).astype(jnp.bfloat16).reshape(num_seqs, seq_len, kv_heads, group_size, head_dim)
    k_rot = rope_apply(k_pre, cos_full, sin_full).astype(jnp.bfloat16)
    score_scale = head_dim ** -0.5
    scores = jnp.einsum('bqkgd,bskd->bkgqs', q_rot, k_rot, preferred_element_type=jnp.float32) * score_scale
    causal = lax.iota(jnp.int32, seq_len)[:, None] >= lax.iota(jnp.int32, seq_len)[None, :]
    attn_probs = jax.nn.softmax(jnp.where(causal, scores, -1e30), axis=-1)
    probs_low = attn_probs.astype(jnp.bfloat16)
    context = jnp.einsum('bkgqs,bskd->bqkgd', probs_low, v_heads, preferred_element_type=jnp.float32).astype(jnp.bfloat16)
    context = context.reshape(n_tok, num_heads * head_dim)
    attn_out = jnp.dot(context, wo_flat, preferred_element_type=jnp.float32)
    hidden = (x_wide + attn_out).astype(jnp.bfloat16)
    inv_two, array_b8 = rms_parts(hidden.astype(jnp.float32))
    gain_two = mlp_gain.astype(jnp.float32)
    normed_mlp = (array_b8 * gain_two).astype(jnp.bfloat16)
    gate_pre = jnp.dot(normed_mlp, w_gate, preferred_element_type=jnp.float32)
    up_pre = jnp.dot(normed_mlp, w_up, preferred_element_type=jnp.float32)
    gate_sig = jax.nn.sigmoid(gate_pre)
    gate_act = gate_pre * gate_sig
    gated_act = (gate_act * up_pre).astype(jnp.bfloat16)
    g_down = jnp.einsum('nf,nd->fd', gated_act, dy_flat, preferred_element_type=jnp.float32)
    d_gated = jnp.einsum('nd,fd->nf', dy_flat, w_down, preferred_element_type=jnp.float32)
    d_up = (d_gated * gate_act).astype(jnp.bfloat16)
    d_gate = (d_gated * up_pre * gate_sig * (1.0 + gate_pre * (1.0 - gate_sig))).astype(jnp.bfloat16)
    g_gate = jnp.einsum('nd,nf->df', normed_mlp, d_gate, preferred_element_type=jnp.float32)
    g_up = jnp.einsum('nd,nf->df', normed_mlp, d_up, preferred_element_type=jnp.float32)
    mlp_units = (as_units(g_down), as_units(g_gate), as_units(g_up))
    mlp_shards = [scatter(g) for g in mlp_units]
    _, d_gate, d_up, halos = lax.optimization_barrier((mlp_units, d_gate, d_up, halos))
    d_normed_mlp = (jnp.einsum('nf,df->nd', d_gate, w_gate, preferred_element_type=jnp.float32)
                    + jnp.einsum('nf,df->nd', d_up, w_up, preferred_element_type=jnp.float32))
    g_mlp_gain = jnp.sum(d_normed_mlp * array_b8, axis=0)
    d_hidden = rms_back(d_normed_mlp, gain_two, inv_two, array_b8) + dy_flat.astype(jnp.float32)
    d_hidden_low = d_hidden.astype(jnp.bfloat16)
    g_out = jnp.einsum('nc,nd->cd', context, d_hidden_low, preferred_element_type=jnp.float32)
    d_context = jnp.einsum('nd,cd->nc', d_hidden_low, wo_flat, preferred_element_type=jnp.float32).astype(jnp.bfloat16)
    d_context = d_context.reshape(num_seqs, seq_len, kv_heads, group_size, head_dim)
    d_probs = jnp.einsum('bqkgd,bskd->bkgqs', d_context, v_heads, preferred_element_type=jnp.float32)
    g_values = jnp.einsum('bkgqs,bqkgd->bskd', probs_low, d_context, preferred_element_type=jnp.float32)
    d_scores = (attn_probs * (d_probs - jnp.sum(d_probs * attn_probs, axis=-1, keepdims=True)) * score_scale).astype(jnp.bfloat16)
    d_q_rot = jnp.einsum('bkgqs,bskd->bqkgd', d_scores, k_rot, preferred_element_type=jnp.float32).reshape(num_seqs, seq_len, num_heads, head_dim)
    d_k_rot = jnp.einsum('bkgqs,bqkgd->bskd', d_scores, q_rot, preferred_element_type=jnp.float32)
    d_q_pre = rope_back(d_q_rot, cos_full, sin_full).astype(jnp.bfloat16).reshape(n_tok, num_heads * head_dim)
    d_k_pre = rope_back(d_k_rot, cos_full, sin_full).astype(jnp.bfloat16).reshape(n_tok, kv_heads * head_dim)
    d_v_pre = g_values.astype(jnp.bfloat16).reshape(n_tok, kv_heads * head_dim)
    g_query = jnp.einsum('nd,nc->dc', normed, d_q_pre, preferred_element_type=jnp.float32)
    g_key = jnp.einsum('nd,nc->dc', normed, d_k_pre, preferred_element_type=jnp.float32)
    g_value = jnp.einsum('nd,nc->dc', normed, d_v_pre, preferred_element_type=jnp.float32)
    d_normed = (jnp.einsum('nc,dc->nd', d_q_pre, wq_flat, preferred_element_type=jnp.float32)
                + jnp.einsum('nc,dc->nd', d_k_pre, wk_flat, preferred_element_type=jnp.float32)
                + jnp.einsum('nc,dc->nd', d_v_pre, wv_flat, preferred_element_type=jnp.float32))
    g_attn_gain = jnp.sum(d_normed * value_a8, axis=0)
    d_x = rms_back(d_normed, gain_one, inv_one, value_a8) + d_hidden
    pad_row = jnp.zeros((1, 128), jnp.bfloat16)
    gain_units = [jnp.concatenate([pad_row, g_gain.astype(jnp.bfloat16).reshape(-1, 128)]) for g_gain in (g_attn_gain, g_mlp_gain)]
    extra = jnp.concatenate([jnp.stack(gain_units), jnp.zeros((DEVS - 2, 8, 128), jnp.bfloat16)])
    att = jnp.concatenate([as_units(g) for g in (g_query, g_key, g_value, g_out)])
    att = jnp.concatenate([att.reshape(DEVS, ATT_UNITS, 8, 128), extra[:, None]], axis=1).reshape(-1, 8, 128)
    att, mlp_shards = lax.optimization_barrier((att, mlp_shards))
    return d_x.astype(jnp.bfloat16).reshape(num_seqs, seq_len, model_dim), jnp.concatenate([scatter(att), mlp_shards[1], mlp_shards[2], mlp_shards[0]]), halos
def adamw_apply(grad_vec, grad_norm, master_vec, mean_vec, var_vec, first_index, model_dim):
    clip_scale = jnp.minimum(1.0, 1.0 / (grad_norm + 1e-6))
    clipped = grad_vec * clip_scale
    new_mean = BETA_ONE * mean_vec + (1.0 - BETA_ONE) * clipped
    new_var = BETA_TWO * var_vec + (1.0 - BETA_TWO) * clipped * clipped
    mean_hat = new_mean / (1.0 - BETA_ONE ** STEP_COUNT)
    var_hat = new_var / (1.0 - BETA_TWO ** STEP_COUNT)
    flat_index = first_index + lax.iota(jnp.int32, master_vec.shape[0])
    is_gain = (flat_index < model_dim) | ((flat_index >= GAIN_TWO) & (flat_index < GAIN_TWO + model_dim))
    decays = jnp.where(is_gain, 0.0, WEIGHT_DECAY)
    new_master = master_vec - LEARN_RATE * (mean_hat / (jnp.sqrt(var_hat) + ADAM_EPS) + decays * master_vec)
    return new_master, new_mean, new_var


def solution(mesh):
    dp_size = mesh.shape['dp']
    ring_up = [(i, i + 1) for i in range(dp_size - 1)]
    ring_down = [(i + 1, i) for i in range(dp_size - 1)]

    def per_device(x_loc, dy_loc, pos_loc, attn_gain, w_query, w_key, w_value, w_out, mlp_gain, w_gate, w_up, w_down, master_loc, mean_loc, var_loc):
        w_list = (attn_gain, w_query, w_key, w_value, w_out, mlp_gain, w_gate, w_up, w_down)
        me = lax.axis_index('dp')
        heads = jnp.stack([s[:HALO] for s in (master_loc, mean_loc, var_loc)])
        tails = jnp.stack([s[BLOCK - HALO:] for s in (master_loc, mean_loc, var_loc)])
        before = lax.ppermute(tails, 'dp', ring_up)
        after = lax.ppermute(heads, 'dp', ring_down)
        grad_x, shard, (before, after) = local_grads(x_loc, dy_loc, pos_loc, w_list, (before, after))
        part = jnp.sum(jnp.square(shard.astype(jnp.float32) / dp_size))
        part = jnp.where(lax.iota(jnp.int32, UNIT).reshape(1, 8, 128) == 0, part, 0.0)
        window, parts = spread(shard, part)
        grad_norm = jnp.sqrt(jnp.sum(parts))
        shift = (BLOCK * me + 128) % UNIT
        length = BLOCK + 2 * HALO
        first_index = BLOCK * me - HALO
        index = first_index + lax.iota(jnp.int32, length)
        flat_win = window.reshape(-1)
        grad_ext = jnp.where(index < GAIN_TWO, lax.dynamic_slice(flat_win, (shift,), (length,)),
                             lax.dynamic_slice(flat_win, (shift + 128,), (length,)))
        grad_ext = grad_ext.astype(jnp.float32) / dp_size
        ext = [jnp.concatenate([before[k], s, after[k]]) for k, s in enumerate((master_loc, mean_loc, var_loc))]
        new_ext = adamw_apply(grad_ext, grad_norm, ext[0], ext[1], ext[2], first_index, attn_gain.shape[0])
        new_state = tuple(s[HALO:HALO + BLOCK] for s in new_ext)
        w_ext = jnp.pad(new_ext[0].astype(jnp.bfloat16), (2048, 8192))
        place = UNIT * (first_unit(me) - HALO_UNITS) + lax.iota(jnp.int32, WINDOW * UNIT)
        w_win = jnp.where(place < GAIN_UNIT * UNIT, lax.dynamic_slice(w_ext, (2048 - shift,), (WINDOW * UNIT,)),
                          lax.dynamic_slice(w_ext, (1920 - shift,), (WINDOW * UNIT,)))
        new_shard = collect(w_win.reshape(WINDOW, 8, 128))
        ends = (0, ATT_UNITS + 1, ATT_UNITS + 1 + MLP_UNITS, ATT_UNITS + 1 + 2 * MLP_UNITS, SHARD)
        full = [lax.all_gather(new_shard[ends[k]:ends[k + 1]], 'dp', tiled=True) for k in range(4)]
        att = full[0].reshape(DEVS, ATT_UNITS + 1, 8, 128)
        gains = [att[k, ATT_UNITS].reshape(-1)[128:] for k in range(2)]
        att = att[:, :ATT_UNITS].reshape(DEVS * ATT_UNITS, 8, 128)
        pieces = []
        offset = 0
        for weight in (w_query, w_key, w_value, w_out):
            pieces.append(att[offset:offset + weight.size // UNIT].reshape(weight.shape))
            offset += weight.size // UNIT
        new_weights = [gains[0]] + pieces + [gains[1], full[1].reshape(w_gate.shape), full[2].reshape(w_up.shape), full[3].reshape(w_down.shape)]
        return (grad_x,) + tuple(new_weights) + new_state + (grad_norm,)

    in_specs = (P('dp'),) * 3 + (P(),) * 9 + (P('dp'),) * 3
    out_specs = (P('dp'),) + (P(),) * 9 + (P('dp'),) * 3 + (P(),)
    return jax.shard_map(per_device, mesh=mesh, in_specs=in_specs, out_specs=out_specs, check_vma=False)
```

```python
import jax
import jax.numpy as jnp
from jax import lax
from jax.experimental import pallas as pl
from jax.experimental.pallas import tpu as pltpu
from jax.sharding import PartitionSpec as P

NORM_EPS = 1e-5
ROPE_BASE = 10000.0
LEARN_RATE = 2e-3
BETA_ONE = 0.9
BETA_TWO = 0.95
ADAM_EPS = 1e-8
WEIGHT_DECAY = 0.1
STEP_COUNT = 100


DEVS = 32
UNIT = 1024
BLOCK = 465976
ATT_UNITS = 56
MLP_UNITS = 133
GAIN_UNIT = 1 + DEVS * ATT_UNITS
MLP_UNIT = GAIN_UNIT + 1
GAIN_TWO = 1835904
ATT_CHUNK = 14
MLP_CHUNK = 19
GAIN_TWO = 1835904
GAIN_OWNER = GAIN_TWO // BLOCK
HALO_UNITS = 20
HALO = HALO_UNITS * UNIT
LEAD = 2048
CORE_UNITS = 457
WINDOW = HALO_UNITS + CORE_UNITS + MLP_CHUNK
SHARD = ATT_UNITS + 1 + 3 * MLP_UNITS
CHIPS = DEVS // 2
SLAB = 38
GU_UNITS = 7 * SLAB
PIECES = ((0, 1, ATT_UNITS, ATT_CHUNK), (ATT_UNITS + 1, MLP_UNIT, MLP_UNITS, MLP_CHUNK),
          (ATT_UNITS + 1 + MLP_UNITS, MLP_UNIT + DEVS * MLP_UNITS, MLP_UNITS, MLP_CHUNK),
          (ATT_UNITS + 1 + 2 * MLP_UNITS, MLP_UNIT + 2 * DEVS * MLP_UNITS, MLP_UNITS, MLP_CHUNK))


def as_units(grad):
    return grad.astype(jnp.bfloat16).reshape(-1, 8, 128)


def scatter(units):
    return lax.psum_scatter(units, 'dp', scatter_dimension=0, tiled=True)


def first_unit(owner):
    return (BLOCK * owner + 128) // UNIT


def last_owner(unit, chunk):
    return jnp.minimum((UNIT * (unit + chunk) - 129) // BLOCK, DEVS - 1)


def first_owner(unit):
    return (jnp.maximum(UNIT * (unit - CORE_UNITS + 1) - 128, 0) + BLOCK - 1) // BLOCK


def start_copy(source, target, peer, me, send_sem, recv_sem):
    @pl.when(peer == me)
    def _():
        pltpu.make_async_copy(source, target, recv_sem).start()

    @pl.when(peer != me)
    def _():
        pltpu.make_async_remote_copy(source, target, send_sem, recv_sem, device_id={'dp': peer}).start()


def end_send(source, target, peer, me, send_sem, recv_sem):
    @pl.when(peer != me)
    def _():
        pltpu.make_async_remote_copy(source, target, send_sem, recv_sem, device_id={'dp': peer}).wait_send()


def end_recv(target, recv_sem):
    pltpu.make_async_copy(target, target, recv_sem).wait()


def reach(unit, base, total, chunk):
    return jnp.minimum(jnp.maximum(unit - base, 0) // chunk, total)


def window_slot(unit, owner):
    return unit - first_unit(owner) + HALO_UNITS


def spread_kernel(shard_ref, part_ref, window_ref, parts_ref, att_send, att_recv, mlp_send, mlp_recv, part_send, part_recv, gain_send, gain_recv):
    me = lax.axis_index('dp')

    def place(unit, owner, size):
        return window_ref.at[pl.ds(window_slot(unit, owner), size)]

    def part_copy(step):
        return pltpu.make_async_remote_copy(part_ref, parts_ref.at[pl.ds(me, 1)], part_send.at[step], part_recv.at[me],
                                            device_id={'dp': lax.rem(me + step, DEVS)})

    def start_part(step, carry):
        part_copy(step).start()
        return carry

    def end_part(step, carry):
        part_copy(step).wait_send()
        return carry

    def take_part(peer, carry):
        end_recv(parts_ref.at[pl.ds(peer, 1)], part_recv.at[peer])
        return carry

    def each_chunk(action):
        first = 0
        for offset, base, count, chunk in PIECES:
            sends, recvs = (att_send, att_recv) if chunk == ATT_CHUNK else (mlp_send, mlp_recv)

            def step(index, carry, offset=offset, base=base, count=count, chunk=chunk, first=first, sends=sends, recvs=recvs):
                source = shard_ref.at[pl.ds(offset + index * chunk, chunk)]
                unit = base + me * count + index * chunk
                low, high = first_owner(unit), last_owner(unit, chunk)
                action(source, place(unit, high, chunk), high, me, sends.at[2 * (first + index)], recvs.at[window_slot(unit, high) // chunk])

                @pl.when(low != high)
                def _():
                    action(source, place(unit, low, chunk), low, me, sends.at[2 * (first + index) + 1],
                           recvs.at[window_slot(unit, low) // chunk])
                return carry
            lax.fori_loop(0, count // chunk, step, 0)
            first = 0 if chunk == ATT_CHUNK else first + count // chunk

    gain_source = shard_ref.at[pl.ds(ATT_UNITS, 1)]
    gain_two = pltpu.make_async_remote_copy(gain_source, place(GAIN_UNIT, GAIN_OWNER, 1), gain_send, gain_recv, device_id={'dp': GAIN_OWNER})
    gain_one = pltpu.make_async_copy(gain_source, place(0, 0, 1), gain_recv)
    pltpu.make_async_copy(part_ref, parts_ref.at[pl.ds(me, 1)], part_recv.at[me]).start()
    lax.fori_loop(1, DEVS, start_part, 0)

    @pl.when(me == 0)
    def _():
        gain_one.start()

    @pl.when(me == 1)
    def _():
        gain_two.start()

    each_chunk(start_copy)
    for base, total, chunk, recvs in ((1, DEVS * ATT_UNITS // ATT_CHUNK, ATT_CHUNK, att_recv),
                                      (MLP_UNIT, 3 * DEVS * MLP_UNITS // MLP_CHUNK, MLP_CHUNK, mlp_recv)):
        def take(index, carry, base=base, chunk=chunk, recvs=recvs):
            unit = base + index * chunk
            end_recv(place(unit, me, chunk), recvs.at[window_slot(unit, me) // chunk])
            return carry
        low = first_unit(me)
        lax.fori_loop(reach(low, base, total, chunk), reach(low + CORE_UNITS + chunk - 1, base, total, chunk), take, 0)
    each_chunk(end_send)
    lax.fori_loop(0, DEVS, take_part, 0)
    lax.fori_loop(1, DEVS, end_part, 0)

    @pl.when(me == 0)
    def _():
        gain_one.wait()

    @pl.when(me == 1)
    def _():
        gain_two.wait_send()

    @pl.when(me == GAIN_OWNER)
    def _():
        end_recv(place(GAIN_UNIT, me, 1), gain_recv)


def collect_kernel(window_ref, att_ref, gu_ref, down_ref, att_send, att_recv, mlp_send, gu_recv, down_recv, gain_send, gain_recv):
    me = lax.axis_index('dp')

    def slot(unit, size):
        return window_ref.at[pl.ds(window_slot(unit, me), size)]

    def even(index, per, target, recvs, chunk):
        peer = index // per
        within = index - peer * per
        return target.at[pl.ds(within * chunk, chunk)], peer, recvs.at[within]

    def slabs(index, cut):
        chip = index // 14
        half = index - chip * 14
        row = half // 2
        core = jnp.where(row >= cut, 1, 0)
        spot = jnp.where(row < 3, row, jnp.where(row == 3, 6, row - 4)) + jnp.where(row == 3, 0, 3 * (4 - cut))
        spot = 2 * spot + half - 2 * row
        return gu_ref.at[pl.ds(spot * MLP_CHUNK, MLP_CHUNK)], 2 * chip + core, gu_recv.at[spot]

    homes = (lambda index: even(index, 4, att_ref, att_recv, ATT_CHUNK), lambda index: slabs(index, 4),
             lambda index: slabs(index, 3), lambda index: even(index, 7, down_ref, down_recv, MLP_CHUNK))

    def each_chunk(action):
        for (_, base, count, chunk), home in zip(PIECES, homes):
            total = DEVS * count // chunk
            sends = att_send if chunk == ATT_CHUNK else mlp_send

            def step(index, carry, base=base, chunk=chunk, home=home, sends=sends):
                unit = base + index * chunk
                target, peer, recv = home(index)
                action(slot(unit, chunk), target, peer, me, sends.at[window_slot(unit, me) // chunk], recv)
                return carry
            high = jnp.where(me == DEVS - 1, total, reach(first_unit(me + 1), base, total, chunk))
            lax.fori_loop(reach(first_unit(me), base, total, chunk), high, step, 0)

    gain_target = att_ref.at[pl.ds(ATT_UNITS, 1)]
    gain_two = pltpu.make_async_remote_copy(slot(GAIN_UNIT, 1), gain_target, gain_send, gain_recv, device_id={'dp': 1})
    gain_one = pltpu.make_async_copy(slot(0, 1), gain_target, gain_recv)

    @pl.when(me == 0)
    def _():
        gain_one.start()

    @pl.when(me == GAIN_OWNER)
    def _():
        gain_two.start()

    each_chunk(start_copy)
    for target, recvs, chunk, count in ((att_ref, att_recv, ATT_CHUNK, 4), (gu_ref, gu_recv, MLP_CHUNK, 14), (down_ref, down_recv, MLP_CHUNK, 7)):
        def take(index, carry, target=target, recvs=recvs, chunk=chunk):
            end_recv(target.at[pl.ds(index * chunk, chunk)], recvs.at[index])
            return carry
        lax.fori_loop(0, count, take, 0)
    each_chunk(end_send)

    @pl.when(me == 0)
    def _():
        gain_one.wait()

    @pl.when(me == GAIN_OWNER)
    def _():
        gain_two.wait_send()

    @pl.when(me == 1)
    def _():
        end_recv(gain_target, gain_recv)


KINDS = 5


def gather_kernel(gu_in, down_in, att_in, gate_ref, up_ref, down_ref, att_ref, z_send, x_send, y_send, mate_send, home_sem, recv_sem, mate_sem):
    me = lax.axis_index('dp')
    core = lax.rem(me, 2)
    x = lax.rem(me // 2, 2)
    y = lax.rem(me // 4, 2)
    z = me // 8
    x_peer, y_peer, mate = me + 2 - 4 * x, me + 4 - 8 * y, me + 1 - 2 * core

    def blocks(chip, side, kind, own, action):
        def run(target, source):
            action(source if own else target, target)
        if kind == 0:
            run(gate_ref.at[pl.ds(7 * chip + 4 * side, 3)], gu_in.at[pl.ds(0, 3)])
        elif kind == 1:
            run(down_ref.at[pl.ds(19 * (2 * chip + side), 19)], down_in)
        elif kind == 2:
            run(up_ref.at[pl.ds(7 * chip + 4 * side, 3)], gu_in.at[pl.ds(3, 3)])
        elif kind == 3:
            run(att_ref.at[pl.ds((ATT_UNITS + 1) * (2 * chip + side), ATT_UNITS + 1)], att_in)
        else:
            @pl.when(side == 0)
            def _():
                run(gate_ref.at[pl.ds(7 * chip + 3, 1)], gu_in.at[pl.ds(6, 1)])

            @pl.when(side == 1)
            def _():
                run(up_ref.at[pl.ds(7 * chip + 3, 1)], gu_in.at[pl.ds(6, 1)])

    pushed = []

    def push(chip, kinds, peer, sends, recvs, own=False, when=None):
        def act(method):
            def body():
                for kind in kinds:
                    def action(source, target, kind=kind):
                        copy = pltpu.make_async_remote_copy(source, target, sends.at[kind], recvs.at[chip, kind], device_id={'dp': peer})
                        getattr(copy, method)()
                    blocks(chip, core, kind, own, action)
            if when is None:
                body()
            else:
                pl.when(when)(body)
        act('start')
        pushed.append(act)

    def take(chip, side, recvs):
        for kind in range(KINDS):
            blocks(chip, side, kind, False, lambda source, target, kind=kind: end_recv(target, recvs.at[chip, kind]))

    def home(method):
        for kind in range(KINDS):
            blocks(me // 2, core, kind, True,
                   lambda source, target, kind=kind: getattr(pltpu.make_async_copy(source, target, home_sem.at[kind]), method)())

    every = tuple(range(KINDS))
    levels = (z, z + 1 - 2 * lax.rem(z, 2), jnp.where(z < 2, 2, 1), jnp.where(z < 2, 3, 0))

    def column(rank):
        level = levels[rank]
        chip = 4 * level + 2 * y + x
        own = rank == 0
        if not own:
            take(chip, core, recv_sem)
        rise, sink = (z < 3, z > 0) if own else ((level < z) & (z < 3), (level > z) & (z > 0))
        push(chip, every, me + 8, z_send.at[rank], recv_sem, own, rise)
        push(chip, every, me - 8, z_send.at[4 + rank], recv_sem, own, sink)
        push(chip, every, x_peer, x_send.at[rank], recv_sem, own)
        push(chip, every, y_peer, y_send.at[rank], recv_sem, own)
        push(chip, every, mate, mate_send.at[rank], mate_sem, own)

    def sides(rank):
        chip = 4 * levels[rank] + 2 * y + (1 - x)
        take(chip, core, recv_sem)
        push(chip, (2, 3, 4), y_peer, y_send.at[4 + rank], recv_sem)
        push(chip, every, mate, mate_send.at[4 + rank], mate_sem)
        chip = 4 * levels[rank] + 2 * (1 - y) + x
        take(chip, core, recv_sem)
        push(chip, (0, 1), x_peer, x_send.at[4 + rank], recv_sem)
        push(chip, every, mate, mate_send.at[8 + rank], mate_sem)

    def corner(rank):
        chip = 4 * levels[rank] + 2 * (1 - y) + (1 - x)
        take(chip, core, recv_sem)
        push(chip, every, mate, mate_send.at[12 + rank], mate_sem)

    home('start')
    for rank in range(6):
        if rank < 4:
            column(rank)
        if 1 <= rank < 5:
            sides(rank - 1)
        if rank >= 2:
            corner(rank - 2)
    home('wait')

    def take_mate(chip, carry):
        take(chip, 1 - core, mate_sem)
        return carry

    lax.fori_loop(0, CHIPS, take_mate, 0)
    for act in pushed:
        act('wait_send')


VMEM = pl.BlockSpec(memory_space=pltpu.VMEM)


DMA = pltpu.SemaphoreType.DMA
PARAMS = pltpu.CompilerParams(has_side_effects=True)


def spread(shard, part):
    return pl.pallas_call(
        spread_kernel,
        out_shape=(jax.ShapeDtypeStruct((WINDOW, 8, 128), jnp.bfloat16), jax.ShapeDtypeStruct((DEVS, 8, 128), jnp.float32)),
        in_specs=[VMEM] * 2, out_specs=(VMEM,) * 2,
        scratch_shapes=[DMA((8,)), DMA((WINDOW // ATT_CHUNK + 1,)), DMA((42,)), DMA((WINDOW // MLP_CHUNK + 1,)), DMA((DEVS,)), DMA((DEVS,)), DMA, DMA],
        compiler_params=PARAMS,
    )(shard, part)


def collect(window):
    return pl.pallas_call(
        collect_kernel,
        out_shape=tuple(jax.ShapeDtypeStruct((units, 8, 128), jnp.bfloat16) for units in (ATT_UNITS + 1, GU_UNITS, MLP_UNITS)),
        in_specs=[VMEM], out_specs=(VMEM,) * 3,
        scratch_shapes=[DMA((WINDOW // ATT_CHUNK + 1,)), DMA((4,)), DMA((WINDOW // MLP_CHUNK + 1,)), DMA((14,)), DMA((7,)), DMA, DMA],
        compiler_params=PARAMS,
    )(window)


def gather(gu_slabs, down_slabs, att_units):
    return pl.pallas_call(
        gather_kernel,
        out_shape=tuple(jax.ShapeDtypeStruct(shape, jnp.bfloat16) for shape in (
            (7 * CHIPS,) + gu_slabs.shape[1:], (7 * CHIPS,) + gu_slabs.shape[1:], (19 * DEVS,) + down_slabs.shape[1:],
            ((ATT_UNITS + 1) * DEVS, 8, 128))),
        in_specs=[VMEM] * 3, out_specs=(pl.BlockSpec(memory_space=pl.ANY),) * 4,
        scratch_shapes=[DMA((8, KINDS)), DMA((8, KINDS)), DMA((8, KINDS)), DMA((16, KINDS)), DMA((KINDS,)), DMA((CHIPS, KINDS)), DMA((CHIPS, KINDS))],
        compiler_params=PARAMS,
    )(gu_slabs, down_slabs, att_units)


def rope_tables(positions, head_dim):
    half_dim = head_dim // 2
    inv_freq = ROPE_BASE ** (-2.0 * jnp.arange(half_dim, dtype=jnp.float32) / head_dim)
    angles = positions.astype(jnp.float32)[:, :, None] * inv_freq
    cos_full = jnp.concatenate([jnp.cos(angles), jnp.cos(angles)], axis=-1)[:, :, None, :]
    sin_full = jnp.concatenate([jnp.sin(angles), jnp.sin(angles)], axis=-1)[:, :, None, :]
    return cos_full, sin_full


def rope_apply(values, cos_full, sin_full):
    half_dim = values.shape[-1] // 2
    rotated = jnp.concatenate([-values[..., half_dim:], values[..., :half_dim]], axis=-1)
    return values * cos_full + rotated * sin_full


def rope_back(grad_rot, cos_full, sin_full):
    half_dim = grad_rot.shape[-1] // 2
    scaled = grad_rot * sin_full
    return grad_rot * cos_full + jnp.concatenate([scaled[..., half_dim:], -scaled[..., :half_dim]], axis=-1)


def rms_parts(values):
    inv_rms = lax.rsqrt(jnp.mean(values * values, axis=-1, keepdims=True) + NORM_EPS)
    return inv_rms, values * inv_rms


def rms_back(d_normed, gain_wide, inv_rms, x_hat):
    d_hat = d_normed * gain_wide
    return inv_rms * (d_hat - x_hat * jnp.mean(d_hat * x_hat, axis=-1, keepdims=True))


def local_grads(x_loc, dy_loc, pos_loc, w_list, halos):
    attn_gain, w_query, w_key, w_value, w_out, mlp_gain, w_gate, w_up, w_down = w_list
    num_seqs, seq_len, model_dim = x_loc.shape
    num_heads, head_dim = w_query.shape[1], w_query.shape[2]
    kv_heads = w_key.shape[1]
    group_size = num_heads // kv_heads
    n_tok = num_seqs * seq_len
    wq_flat = w_query.reshape(model_dim, num_heads * head_dim)
    wk_flat = w_key.reshape(model_dim, kv_heads * head_dim)
    wv_flat = w_value.reshape(model_dim, kv_heads * head_dim)
    wo_flat = w_out.reshape(num_heads * head_dim, model_dim)
    dy_flat = dy_loc.reshape(n_tok, model_dim)
    x_wide = x_loc.reshape(n_tok, model_dim).astype(jnp.float32)
    inv_one, value_a8 = rms_parts(x_wide)
    gain_one = attn_gain.astype(jnp.float32)
    normed = (value_a8 * gain_one).astype(jnp.bfloat16)
    q_pre = jnp.dot(normed, wq_flat, preferred_element_type=jnp.float32).reshape(num_seqs, seq_len, num_heads, head_dim)
    k_pre = jnp.dot(normed, wk_flat, preferred_element_type=jnp.float32).reshape(num_seqs, seq_len, kv_heads, head_dim)
    v_heads = jnp.dot(normed, wv_flat, preferred_element_type=jnp.float32).astype(jnp.bfloat16).reshape(num_seqs, seq_len, kv_heads, head_dim)
    cos_full, sin_full = rope_tables(pos_loc, head_dim)
    q_rot = rope_apply(q_pre, cos_full, sin_full).astype(jnp.bfloat16).reshape(num_seqs, seq_len, kv_heads, group_size, head_dim)
    k_rot = rope_apply(k_pre, cos_full, sin_full).astype(jnp.bfloat16)
    score_scale = head_dim ** -0.5
    scores = jnp.einsum('bqkgd,bskd->bkgqs', q_rot, k_rot, preferred_element_type=jnp.float32) * score_scale
    causal = lax.iota(jnp.int32, seq_len)[:, None] >= lax.iota(jnp.int32, seq_len)[None, :]
    attn_probs = jax.nn.softmax(jnp.where(causal, scores, -1e30), axis=-1)
    probs_low = attn_probs.astype(jnp.bfloat16)
    context = jnp.einsum('bkgqs,bskd->bqkgd', probs_low, v_heads, preferred_element_type=jnp.float32).astype(jnp.bfloat16)
    context = context.reshape(n_tok, num_heads * head_dim)
    attn_out = jnp.dot(context, wo_flat, preferred_element_type=jnp.float32)
    hidden = (x_wide + attn_out).astype(jnp.bfloat16)
    inv_two, array_b8 = rms_parts(hidden.astype(jnp.float32))
    gain_two = mlp_gain.astype(jnp.float32)
    normed_mlp = (array_b8 * gain_two).astype(jnp.bfloat16)
    gate_pre = jnp.dot(normed_mlp, w_gate, preferred_element_type=jnp.float32)
    up_pre = jnp.dot(normed_mlp, w_up, preferred_element_type=jnp.float32)
    gate_sig = jax.nn.sigmoid(gate_pre)
    gate_act = gate_pre * gate_sig
    gated_act = (gate_act * up_pre).astype(jnp.bfloat16)
    g_down = jnp.einsum('nf,nd->fd', gated_act, dy_flat, preferred_element_type=jnp.float32)
    d_gated = jnp.einsum('nd,fd->nf', dy_flat, w_down, preferred_element_type=jnp.float32)
    d_up = (d_gated * gate_act).astype(jnp.bfloat16)
    d_gate = (d_gated * up_pre * gate_sig * (1.0 + gate_pre * (1.0 - gate_sig))).astype(jnp.bfloat16)
    g_gate = jnp.einsum('nd,nf->df', normed_mlp, d_gate, preferred_element_type=jnp.float32)
    g_up = jnp.einsum('nd,nf->df', normed_mlp, d_up, preferred_element_type=jnp.float32)
    mlp_units = (as_units(g_down), as_units(g_gate), as_units(g_up))
    mlp_shards = [scatter(g) for g in mlp_units]
    _, d_gate, d_up, halos = lax.optimization_barrier((mlp_units, d_gate, d_up, halos))
    d_normed_mlp = (jnp.einsum('nf,df->nd', d_gate, w_gate, preferred_element_type=jnp.float32)
                    + jnp.einsum('nf,df->nd', d_up, w_up, preferred_element_type=jnp.float32))
    g_mlp_gain = jnp.sum(d_normed_mlp * array_b8, axis=0)
    d_hidden = rms_back(d_normed_mlp, gain_two, inv_two, array_b8) + dy_flat.astype(jnp.float32)
    d_hidden_low = d_hidden.astype(jnp.bfloat16)
    g_out = jnp.einsum('nc,nd->cd', context, d_hidden_low, preferred_element_type=jnp.float32)
    d_context = jnp.einsum('nd,cd->nc', d_hidden_low, wo_flat, preferred_element_type=jnp.float32).astype(jnp.bfloat16)
    d_context = d_context.reshape(num_seqs, seq_len, kv_heads, group_size, head_dim)
    d_probs = jnp.einsum('bqkgd,bskd->bkgqs', d_context, v_heads, preferred_element_type=jnp.float32)
    g_values = jnp.einsum('bkgqs,bqkgd->bskd', probs_low, d_context, preferred_element_type=jnp.float32)
    d_scores = (attn_probs * (d_probs - jnp.sum(d_probs * attn_probs, axis=-1, keepdims=True)) * score_scale).astype(jnp.bfloat16)
    d_q_rot = jnp.einsum('bkgqs,bskd->bqkgd', d_scores, k_rot, preferred_element_type=jnp.float32).reshape(num_seqs, seq_len, num_heads, head_dim)
    d_k_rot = jnp.einsum('bkgqs,bqkgd->bskd', d_scores, q_rot, preferred_element_type=jnp.float32)
    d_q_pre = rope_back(d_q_rot, cos_full, sin_full).astype(jnp.bfloat16).reshape(n_tok, num_heads * head_dim)
    d_k_pre = rope_back(d_k_rot, cos_full, sin_full).astype(jnp.bfloat16).reshape(n_tok, kv_heads * head_dim)
    d_v_pre = g_values.astype(jnp.bfloat16).reshape(n_tok, kv_heads * head_dim)
    g_query = jnp.einsum('nd,nc->dc', normed, d_q_pre, preferred_element_type=jnp.float32)
    g_key = jnp.einsum('nd,nc->dc', normed, d_k_pre, preferred_element_type=jnp.float32)
    g_value = jnp.einsum('nd,nc->dc', normed, d_v_pre, preferred_element_type=jnp.float32)
    d_normed = (jnp.einsum('nc,dc->nd', d_q_pre, wq_flat, preferred_element_type=jnp.float32)
                + jnp.einsum('nc,dc->nd', d_k_pre, wk_flat, preferred_element_type=jnp.float32)
                + jnp.einsum('nc,dc->nd', d_v_pre, wv_flat, preferred_element_type=jnp.float32))
    g_attn_gain = jnp.sum(d_normed * value_a8, axis=0)
    d_x = rms_back(d_normed, gain_one, inv_one, value_a8) + d_hidden
    pad_row = jnp.zeros((1, 128), jnp.bfloat16)
    gain_units = [jnp.concatenate([pad_row, g_gain.astype(jnp.bfloat16).reshape(-1, 128)]) for g_gain in (g_attn_gain, g_mlp_gain)]
    extra = jnp.concatenate([jnp.stack(gain_units), jnp.zeros((DEVS - 2, 8, 128), jnp.bfloat16)])
    att = jnp.concatenate([as_units(g) for g in (g_query, g_key, g_value, g_out)])
    att = jnp.concatenate([att.reshape(DEVS, ATT_UNITS, 8, 128), extra[:, None]], axis=1).reshape(-1, 8, 128)
    att, mlp_shards = lax.optimization_barrier((att, mlp_shards))
    return d_x.astype(jnp.bfloat16).reshape(num_seqs, seq_len, model_dim), jnp.concatenate([scatter(att), mlp_shards[1], mlp_shards[2], mlp_shards[0]]), halos
def adamw_apply(grad_vec, grad_norm, master_vec, mean_vec, var_vec, first_index, model_dim):
    clip_scale = jnp.minimum(1.0, 1.0 / (grad_norm + 1e-6))
    clipped = grad_vec * clip_scale
    new_mean = BETA_ONE * mean_vec + (1.0 - BETA_ONE) * clipped
    new_var = BETA_TWO * var_vec + (1.0 - BETA_TWO) * clipped * clipped
    mean_hat = new_mean / (1.0 - BETA_ONE ** STEP_COUNT)
    var_hat = new_var / (1.0 - BETA_TWO ** STEP_COUNT)
    flat_index = first_index + lax.iota(jnp.int32, master_vec.shape[0])
    is_gain = (flat_index < model_dim) | ((flat_index >= GAIN_TWO) & (flat_index < GAIN_TWO + model_dim))
    decays = jnp.where(is_gain, 0.0, WEIGHT_DECAY)
    new_master = master_vec - LEARN_RATE * (mean_hat / (jnp.sqrt(var_hat) + ADAM_EPS) + decays * master_vec)
    return new_master, new_mean, new_var


def solution(mesh):
    dp_size = mesh.shape['dp']
    ring_up = [(i, i + 1) for i in range(dp_size - 1)]

    def per_device(x_loc, dy_loc, pos_loc, attn_gain, w_query, w_key, w_value, w_out, mlp_gain, w_gate, w_up, w_down, master_loc, mean_loc, var_loc):
        w_list = (attn_gain, w_query, w_key, w_value, w_out, mlp_gain, w_gate, w_up, w_down)
        me = lax.axis_index('dp')
        state = (master_loc, mean_loc, var_loc)
        halo = lax.ppermute(jnp.stack([vec[BLOCK - HALO:] for vec in state]), 'dp', ring_up)
        grad_x, shard, halo = local_grads(x_loc, dy_loc, pos_loc, w_list, halo)
        part = jnp.sum(jnp.square(shard.astype(jnp.float32) / dp_size))
        part = jnp.where(lax.iota(jnp.int32, UNIT).reshape(1, 8, 128) == 0, part, 0.0)
        window, parts = spread(shard, part)
        grad_norm = jnp.sqrt(jnp.sum(parts))
        shift = (BLOCK * me + 128) % UNIT
        flat_win = window.reshape(-1)

        def update(first, length, vecs):
            index = BLOCK * me - HALO + first + lax.iota(jnp.int32, length)
            grads = jnp.where(index < GAIN_TWO, lax.dynamic_slice(flat_win, (shift + first,), (length,)),
                              lax.dynamic_slice(flat_win, (shift + first + 128,), (length,)))
            return adamw_apply(grads.astype(jnp.float32) / dp_size, grad_norm, vecs[0], vecs[1], vecs[2],
                               BLOCK * me - HALO + first, attn_gain.shape[0])
        new_state = update(HALO, BLOCK, state)
        low_main = new_state[0].astype(jnp.bfloat16)
        low_halo = update(0, HALO, halo)[0].astype(jnp.bfloat16)
        w_ext = jnp.pad(low_main, (LEAD + HALO, WINDOW * UNIT - BLOCK - HALO))
        w_ext = lax.dynamic_update_slice(w_ext, low_halo, (LEAD,))
        place = UNIT * (first_unit(me) - HALO_UNITS) + lax.iota(jnp.int32, WINDOW * UNIT)
        w_win = jnp.where(place < GAIN_UNIT * UNIT, lax.dynamic_slice(w_ext, (LEAD - shift,), (WINDOW * UNIT,)),
                          lax.dynamic_slice(w_ext, (LEAD - 128 - shift,), (WINDOW * UNIT,)))
        att_new, gu_new, down_new = collect(w_win.reshape(WINDOW, 8, 128))
        full = gather(gu_new.reshape(7, 8, w_gate.shape[1]), down_new.reshape(19, 8, w_down.shape[1]), att_new)
        full = (full[3],) + full[:3]
        att = full[0].reshape(DEVS, ATT_UNITS + 1, 8, 128)
        gains = [att[k, ATT_UNITS].reshape(-1)[128:] for k in range(2)]
        att = att[:, :ATT_UNITS].reshape(DEVS * ATT_UNITS, 8, 128)
        pieces = []
        offset = 0
        for weight in (w_query, w_key, w_value, w_out):
            pieces.append(att[offset:offset + weight.size // UNIT].reshape(weight.shape))
            offset += weight.size // UNIT
        new_weights = [gains[0]] + pieces + [gains[1], full[1].reshape(w_gate.shape), full[2].reshape(w_up.shape), full[3].reshape(w_down.shape)]
        return (grad_x,) + tuple(new_weights) + new_state + (grad_norm,)

    in_specs = (P('dp'),) * 3 + (P(),) * 9 + (P('dp'),) * 3
    out_specs = (P('dp'),) + (P(),) * 9 + (P('dp'),) * 3 + (P(),)
    return jax.shard_map(per_device, mesh=mesh, in_specs=in_specs, out_specs=out_specs, check_vma=False)
```

```python
import jax
import jax.numpy as jnp
from jax import lax
from jax.experimental import pallas as pl
from jax.experimental.pallas import tpu as pltpu
from jax.sharding import PartitionSpec as P

NORM_EPS = 1e-5
ROPE_BASE = 10000.0
LEARN_RATE = 2e-3
BETA_ONE = 0.9
BETA_TWO = 0.95
ADAM_EPS = 1e-8
WEIGHT_DECAY = 0.1
STEP_COUNT = 100


DEVS = 32
UNIT = 1024
BLOCK = 465976
ATT_UNITS = 56
MLP_UNITS = 133
GAIN_UNIT = 1 + DEVS * ATT_UNITS
MLP_UNIT = GAIN_UNIT + 1
GAIN_TWO = 1835904
ATT_CHUNK = 14
MLP_CHUNK = 19
GAIN_TWO = 1835904
GAIN_OWNER = GAIN_TWO // BLOCK
HALO_UNITS = 20
HALO = HALO_UNITS * UNIT
LEAD = 2048
CORE_UNITS = 457
WINDOW = HALO_UNITS + CORE_UNITS + MLP_CHUNK
SHARD = ATT_UNITS + 1 + 3 * MLP_UNITS
CHIPS = DEVS // 2
SLAB = 38
GU_UNITS = 7 * SLAB
PIECES = ((0, 1, ATT_UNITS, ATT_CHUNK), (ATT_UNITS + 1, MLP_UNIT, MLP_UNITS, MLP_CHUNK),
          (ATT_UNITS + 1 + MLP_UNITS, MLP_UNIT + DEVS * MLP_UNITS, MLP_UNITS, MLP_CHUNK),
          (ATT_UNITS + 1 + 2 * MLP_UNITS, MLP_UNIT + 2 * DEVS * MLP_UNITS, MLP_UNITS, MLP_CHUNK))


def as_units(grad):
    return grad.astype(jnp.bfloat16).reshape(-1, 8, 128)


def scatter(units):
    return lax.psum_scatter(units, 'dp', scatter_dimension=0, tiled=True)


def first_unit(owner):
    return (BLOCK * owner + 128) // UNIT


def last_owner(unit, chunk):
    return jnp.minimum((UNIT * (unit + chunk) - 129) // BLOCK, DEVS - 1)


def first_owner(unit):
    return (jnp.maximum(UNIT * (unit - CORE_UNITS + 1) - 128, 0) + BLOCK - 1) // BLOCK


def start_copy(source, target, peer, me, send_sem, recv_sem):
    @pl.when(peer == me)
    def _():
        pltpu.make_async_copy(source, target, recv_sem).start()

    @pl.when(peer != me)
    def _():
        pltpu.make_async_remote_copy(source, target, send_sem, recv_sem, device_id={'dp': peer}).start()


def end_send(source, target, peer, me, send_sem, recv_sem):
    @pl.when(peer != me)
    def _():
        pltpu.make_async_remote_copy(source, target, send_sem, recv_sem, device_id={'dp': peer}).wait_send()


def end_recv(target, recv_sem):
    pltpu.make_async_copy(target, target, recv_sem).wait()


def reach(unit, base, total, chunk):
    return jnp.minimum(jnp.maximum(unit - base, 0) // chunk, total)


def window_slot(unit, owner):
    return unit - first_unit(owner) + HALO_UNITS


def spread_kernel(shard_ref, part_ref, window_ref, parts_ref, att_send, att_recv, mlp_send, mlp_recv, part_send, part_recv, gain_send, gain_recv):
    me = lax.axis_index('dp')

    def place(unit, owner, size):
        return window_ref.at[pl.ds(window_slot(unit, owner), size)]

    def part_copy(step):
        return pltpu.make_async_remote_copy(part_ref, parts_ref.at[pl.ds(me, 1)], part_send.at[step], part_recv.at[me],
                                            device_id={'dp': lax.rem(me + step, DEVS)})

    def start_part(step, carry):
        part_copy(step).start()
        return carry

    def end_part(step, carry):
        part_copy(step).wait_send()
        return carry

    def take_part(peer, carry):
        end_recv(parts_ref.at[pl.ds(peer, 1)], part_recv.at[peer])
        return carry

    def each_chunk(action):
        first = 0
        for offset, base, count, chunk in PIECES:
            sends, recvs = (att_send, att_recv) if chunk == ATT_CHUNK else (mlp_send, mlp_recv)

            def step(index, carry, offset=offset, base=base, count=count, chunk=chunk, first=first, sends=sends, recvs=recvs):
                source = shard_ref.at[pl.ds(offset + index * chunk, chunk)]
                unit = base + me * count + index * chunk
                low, high = first_owner(unit), last_owner(unit, chunk)
                action(source, place(unit, high, chunk), high, me, sends.at[2 * (first + index)], recvs.at[window_slot(unit, high) // chunk])

                @pl.when(low != high)
                def _():
                    action(source, place(unit, low, chunk), low, me, sends.at[2 * (first + index) + 1],
                           recvs.at[window_slot(unit, low) // chunk])
                return carry
            lax.fori_loop(0, count // chunk, step, 0)
            first = 0 if chunk == ATT_CHUNK else first + count // chunk

    gain_source = shard_ref.at[pl.ds(ATT_UNITS, 1)]
    gain_two = pltpu.make_async_remote_copy(gain_source, place(GAIN_UNIT, GAIN_OWNER, 1), gain_send, gain_recv, device_id={'dp': GAIN_OWNER})
    gain_one = pltpu.make_async_copy(gain_source, place(0, 0, 1), gain_recv)
    pltpu.make_async_copy(part_ref, parts_ref.at[pl.ds(me, 1)], part_recv.at[me]).start()
    lax.fori_loop(1, DEVS, start_part, 0)

    @pl.when(me == 0)
    def _():
        gain_one.start()

    @pl.when(me == 1)
    def _():
        gain_two.start()

    each_chunk(start_copy)
    for base, total, chunk, recvs in ((1, DEVS * ATT_UNITS // ATT_CHUNK, ATT_CHUNK, att_recv),
                                      (MLP_UNIT, 3 * DEVS * MLP_UNITS // MLP_CHUNK, MLP_CHUNK, mlp_recv)):
        def take(index, carry, base=base, chunk=chunk, recvs=recvs):
            unit = base + index * chunk
            end_recv(place(unit, me, chunk), recvs.at[window_slot(unit, me) // chunk])
            return carry
        low = first_unit(me)
        lax.fori_loop(reach(low, base, total, chunk), reach(low + CORE_UNITS + chunk - 1, base, total, chunk), take, 0)
    each_chunk(end_send)
    lax.fori_loop(0, DEVS, take_part, 0)
    lax.fori_loop(1, DEVS, end_part, 0)

    @pl.when(me == 0)
    def _():
        gain_one.wait()

    @pl.when(me == 1)
    def _():
        gain_two.wait_send()

    @pl.when(me == GAIN_OWNER)
    def _():
        end_recv(place(GAIN_UNIT, me, 1), gain_recv)


def collect_kernel(window_ref, att_ref, gu_ref, down_ref, att_send, att_recv, mlp_send, gu_recv, down_recv, gain_send, gain_recv):
    me = lax.axis_index('dp')

    def slot(unit, size):
        return window_ref.at[pl.ds(window_slot(unit, me), size)]

    def even(index, per, target, recvs, chunk):
        peer = index // per
        within = index - peer * per
        return target.at[pl.ds(within * chunk, chunk)], peer, recvs.at[within]

    def slabs(index, cut):
        chip = index // 14
        half = index - chip * 14
        row = half // 2
        core = jnp.where(row >= cut, 1, 0)
        spot = jnp.where(row < 3, row, jnp.where(row == 3, 6, row - 4)) + jnp.where(row == 3, 0, 3 * (4 - cut))
        spot = 2 * spot + half - 2 * row
        return gu_ref.at[pl.ds(spot * MLP_CHUNK, MLP_CHUNK)], 2 * chip + core, gu_recv.at[spot]

    homes = (lambda index: even(index, 4, att_ref, att_recv, ATT_CHUNK), lambda index: slabs(index, 4),
             lambda index: slabs(index, 3), lambda index: even(index, 7, down_ref, down_recv, MLP_CHUNK))

    def each_chunk(action):
        for (_, base, count, chunk), home in zip(PIECES, homes):
            total = DEVS * count // chunk
            sends = att_send if chunk == ATT_CHUNK else mlp_send

            def step(index, carry, base=base, chunk=chunk, home=home, sends=sends):
                unit = base + index * chunk
                target, peer, recv = home(index)
                action(slot(unit, chunk), target, peer, me, sends.at[window_slot(unit, me) // chunk], recv)
                return carry
            high = jnp.where(me == DEVS - 1, total, reach(first_unit(me + 1), base, total, chunk))
            lax.fori_loop(reach(first_unit(me), base, total, chunk), high, step, 0)

    gain_target = att_ref.at[pl.ds(ATT_UNITS, 1)]
    gain_two = pltpu.make_async_remote_copy(slot(GAIN_UNIT, 1), gain_target, gain_send, gain_recv, device_id={'dp': 1})
    gain_one = pltpu.make_async_copy(slot(0, 1), gain_target, gain_recv)

    @pl.when(me == 0)
    def _():
        gain_one.start()

    @pl.when(me == GAIN_OWNER)
    def _():
        gain_two.start()

    each_chunk(start_copy)
    for target, recvs, chunk, count in ((att_ref, att_recv, ATT_CHUNK, 4), (gu_ref, gu_recv, MLP_CHUNK, 14), (down_ref, down_recv, MLP_CHUNK, 7)):
        def take(index, carry, target=target, recvs=recvs, chunk=chunk):
            end_recv(target.at[pl.ds(index * chunk, chunk)], recvs.at[index])
            return carry
        lax.fori_loop(0, count, take, 0)
    each_chunk(end_send)

    @pl.when(me == 0)
    def _():
        gain_one.wait()

    @pl.when(me == GAIN_OWNER)
    def _():
        gain_two.wait_send()

    @pl.when(me == 1)
    def _():
        end_recv(gain_target, gain_recv)


KINDS = 5


def gather_kernel(gu_in, down_in, att_in, gate_ref, up_ref, down_ref, att_ref, z_send, x_send, y_send, mate_send, home_sem, recv_sem, mate_sem):
    me = lax.axis_index('dp')
    core = lax.rem(me, 2)
    x = lax.rem(me // 2, 2)
    y = lax.rem(me // 4, 2)
    z = me // 8
    x_peer, y_peer, mate = me + 2 - 4 * x, me + 4 - 8 * y, me + 1 - 2 * core

    def blocks(chip, side, kind, own, action):
        def run(target, source):
            action(source if own else target, target)
        if kind == 0:
            run(gate_ref.at[pl.ds(7 * chip + 4 * side, 3)], gu_in.at[pl.ds(0, 3)])
        elif kind == 1:
            run(down_ref.at[pl.ds(19 * (2 * chip + side), 19)], down_in)
        elif kind == 2:
            run(up_ref.at[pl.ds(7 * chip + 4 * side, 3)], gu_in.at[pl.ds(3, 3)])
        elif kind == 3:
            run(att_ref.at[pl.ds((ATT_UNITS + 1) * (2 * chip + side), ATT_UNITS + 1)], att_in)
        else:
            @pl.when(side == 0)
            def _():
                run(gate_ref.at[pl.ds(7 * chip + 3, 1)], gu_in.at[pl.ds(6, 1)])

            @pl.when(side == 1)
            def _():
                run(up_ref.at[pl.ds(7 * chip + 3, 1)], gu_in.at[pl.ds(6, 1)])

    pushed = []

    def push(chip, kinds, peer, sends, recvs, own=False, when=None):
        def act(method):
            def body():
                for kind in kinds:
                    def action(source, target, kind=kind):
                        copy = pltpu.make_async_remote_copy(source, target, sends.at[kind], recvs.at[chip, kind], device_id={'dp': peer})
                        getattr(copy, method)()
                    blocks(chip, core, kind, own, action)
            if when is None:
                body()
            else:
                pl.when(when)(body)
        act('start')
        pushed.append(act)

    def take(chip, side, recvs):
        for kind in range(KINDS):
            blocks(chip, side, kind, False, lambda source, target, kind=kind: end_recv(target, recvs.at[chip, kind]))

    def home(method):
        for kind in range(KINDS):
            blocks(me // 2, core, kind, True,
                   lambda source, target, kind=kind: getattr(pltpu.make_async_copy(source, target, home_sem.at[kind]), method)())

    every = tuple(range(KINDS))
    levels = (z, z + 1 - 2 * lax.rem(z, 2), jnp.where(z < 2, 2, 1), jnp.where(z < 2, 3, 0))

    def column(rank):
        level = levels[rank]
        chip = 4 * level + 2 * y + x
        own = rank == 0
        if not own:
            take(chip, core, recv_sem)
        rise, sink = (z < 3, z > 0) if own else ((level < z) & (z < 3), (level > z) & (z > 0))
        push(chip, every, me + 8, z_send.at[rank], recv_sem, own, rise)
        push(chip, every, me - 8, z_send.at[4 + rank], recv_sem, own, sink)
        push(chip, every, x_peer, x_send.at[rank], recv_sem, own)
        push(chip, every, y_peer, y_send.at[rank], recv_sem, own)
        push(chip, every, mate, mate_send.at[rank], mate_sem, own)

    def sides(rank):
        chip = 4 * levels[rank] + 2 * y + (1 - x)
        take(chip, core, recv_sem)
        push(chip, (2, 3, 4), y_peer, y_send.at[4 + rank], recv_sem)
        push(chip, every, mate, mate_send.at[4 + rank], mate_sem)
        chip = 4 * levels[rank] + 2 * (1 - y) + x
        take(chip, core, recv_sem)
        push(chip, (0, 1), x_peer, x_send.at[4 + rank], recv_sem)
        push(chip, every, mate, mate_send.at[8 + rank], mate_sem)

    def corner(rank):
        chip = 4 * levels[rank] + 2 * (1 - y) + (1 - x)
        take(chip, core, recv_sem)
        push(chip, every, mate, mate_send.at[12 + rank], mate_sem)

    home('start')
    for rank in range(6):
        if rank < 4:
            column(rank)
        if 1 <= rank < 5:
            sides(rank - 1)
        if rank >= 2:
            corner(rank - 2)
    home('wait')

    def take_mate(chip, carry):
        take(chip, 1 - core, mate_sem)
        return carry

    lax.fori_loop(0, CHIPS, take_mate, 0)
    for act in pushed:
        act('wait_send')


VMEM = pl.BlockSpec(memory_space=pltpu.VMEM)


LATE = MLP_UNITS + ATT_UNITS + 1
CUT = LATE // 2


def reduce_kernel(up_ref, att_ref, out_ref, pair, first, second, below, above, pair_send, pair_recv, a_send, a_recv, b_send, b_recv,
                  c_send, c_recv, d_send, d_recv, z_send, below_recv, above_recv):
    me = lax.axis_index('dp')
    core = lax.rem(me, 2)
    x = lax.rem(me // 2, 2)
    y = lax.rem(me // 4, 2)
    z = me // 8
    x_peer, y_peer, mate = me + 2 - 4 * x, me + 4 - 8 * y, me + 1 - 2 * core
    near = lax.rem(z, 2)
    levels = (jnp.where(z < 2, 3, 0), jnp.where(z < 2, 2, 1), z + 1 - 2 * near, z)
    halves = (pl.ds(0, CUT), pl.ds(CUT, CUT))

    def remote(source, target, send, recv, peer):
        return pltpu.make_async_remote_copy(source, target, send, recv, device_id={'dp': peer})

    def pair_copies(rank):
        level = levels[rank]
        chips = pl.ds(4 * level, 4)
        return (remote(up_ref.at[chips, 1 - core], pair.at[level, :, pl.ds(0, MLP_UNITS)], pair_send.at[rank, 0], pair_recv.at[rank, 0], mate),
                remote(att_ref.at[chips, 1 - core], pair.at[level, :, pl.ds(MLP_UNITS, ATT_UNITS + 1)], pair_send.at[rank, 1],
                       pair_recv.at[rank, 1], mate))

    def a_copies(rank):
        level = levels[rank]
        return [remote(pair.at[level, 2 * side + 1 - x, halves[0]], first.at[level, side, halves[0]], a_send.at[rank, side],
                       a_recv.at[rank, side], x_peer) for side in range(2)]

    def b_copies(rank):
        level = levels[rank]
        return [remote(pair.at[level, 2 * (1 - y) + side, halves[1]], first.at[level, side, halves[1]], b_send.at[rank, side],
                       b_recv.at[rank, side], y_peer) for side in range(2)]

    def c_copy(rank):
        level = levels[rank]
        return remote(first.at[level, 1 - y, halves[0]], second.at[level, halves[0]], c_send.at[rank], c_recv.at[rank], y_peer)

    def d_copy(rank):
        level = levels[rank]
        return remote(first.at[level, 1 - x, halves[1]], second.at[level, halves[1]], d_send.at[rank], d_recv.at[rank], x_peer)

    def up_copy(rank):
        level = levels[rank]
        return remote(second.at[level], below.at[level], z_send.at[rank], below_recv.at[level], me + 8)

    def down_copy(rank):
        level = levels[rank]
        return remote(second.at[level], above.at[level], z_send.at[rank], above_recv.at[level], me - 8)

    def add(target, source, count, step=19):
        def body(index, carry):
            rows = pl.ds(index * step, step)
            target[rows] = (target[rows].astype(jnp.float32) + source[rows].astype(jnp.float32)).astype(jnp.bfloat16)
            return carry
        lax.fori_loop(0, count // step, body, 0)

    def begin(rank):
        level = levels[rank]
        for copy in pair_copies(rank):
            copy.wait_recv()
        for chip in range(4):
            add(pair.at[level, chip, pl.ds(0, MLP_UNITS)], up_ref.at[4 * level + chip, core], MLP_UNITS)
            add(pair.at[level, chip, pl.ds(MLP_UNITS, ATT_UNITS + 1)], att_ref.at[4 * level + chip, core], ATT_UNITS + 1)
        for copy in a_copies(rank) + b_copies(rank):
            copy.start()

    def middle(rank):
        level = levels[rank]
        for copy in a_copies(rank) + b_copies(rank):
            copy.wait_recv()
        for side in range(2):
            add(first.at[level, side, halves[0]], pair.at[level, 2 * side + x, halves[0]], CUT)
            add(first.at[level, side, halves[1]], pair.at[level, 2 * y + side, halves[1]], CUT)
        c_copy(rank).start()
        d_copy(rank).start()

    def climb(rank):
        level = levels[rank]
        c_copy(rank).wait_recv()
        d_copy(rank).wait_recv()
        add(second.at[level, halves[0]], first.at[level, y, halves[0]], CUT)
        add(second.at[level, halves[1]], first.at[level, x, halves[1]], CUT)
        rising = (level >= z) & (z > 0)
        sinking = (level <= z) & (z < 3)

        @pl.when(rising)
        def _():
            pltpu.make_async_copy(below.at[level], below.at[level], below_recv.at[level]).wait()
            add(second.at[level], below.at[level], LATE)

        @pl.when(sinking)
        def _():
            pltpu.make_async_copy(above.at[level], above.at[level], above_recv.at[level]).wait()
            add(second.at[level], above.at[level], LATE)

        if rank < 3:
            @pl.when(level > z)
            def _():
                up_copy(rank).start()

            @pl.when(level < z)
            def _():
                down_copy(rank).start()
        else:
            def body(index, carry):
                rows = pl.ds(index * 19, 19)
                out_ref[rows] = second[level, rows]
                return carry
            lax.fori_loop(0, LATE // 19, body, 0)

    for rank in range(4):
        for copy in pair_copies(rank):
            copy.start()
    for step in range(6):
        if step < 4:
            begin(step)
        if 1 <= step < 5:
            middle(step - 1)
        if step >= 2:
            climb(step - 2)
    for rank in range(4):
        for copy in list(pair_copies(rank)) + a_copies(rank) + b_copies(rank) + [c_copy(rank), d_copy(rank)]:
            copy.wait_send()
    for rank in range(3):
        @pl.when(levels[rank] > z)
        def _(rank=rank):
            up_copy(rank).wait_send()

        @pl.when(levels[rank] < z)
        def _(rank=rank):
            down_copy(rank).wait_send()


DMA = pltpu.SemaphoreType.DMA
PARAMS = pltpu.CompilerParams(has_side_effects=True)


def reduce_late(up_units, att_units):
    shape = (8, 128)
    return pl.pallas_call(
        reduce_kernel,
        out_shape=jax.ShapeDtypeStruct((LATE,) + shape, jnp.bfloat16),
        in_specs=[VMEM] * 2, out_specs=VMEM,
        scratch_shapes=[pltpu.VMEM(dims + (LATE,) + shape, jnp.bfloat16) for dims in ((4, 4), (4, 2), (4,), (4,), (4,))]
        + [DMA((4, 2))] * 6 + [DMA((4,))] * 7,
        compiler_params=PARAMS,
    )(up_units.reshape((CHIPS, 2, MLP_UNITS) + shape), att_units.reshape((CHIPS, 2, ATT_UNITS + 1) + shape))


def spread(shard, part):
    return pl.pallas_call(
        spread_kernel,
        out_shape=(jax.ShapeDtypeStruct((WINDOW, 8, 128), jnp.bfloat16), jax.ShapeDtypeStruct((DEVS, 8, 128), jnp.float32)),
        in_specs=[VMEM] * 2, out_specs=(VMEM,) * 2,
        scratch_shapes=[DMA((8,)), DMA((WINDOW // ATT_CHUNK + 1,)), DMA((42,)), DMA((WINDOW // MLP_CHUNK + 1,)), DMA((DEVS,)), DMA((DEVS,)), DMA, DMA],
        compiler_params=PARAMS,
    )(shard, part)


def collect(window):
    return pl.pallas_call(
        collect_kernel,
        out_shape=tuple(jax.ShapeDtypeStruct((units, 8, 128), jnp.bfloat16) for units in (ATT_UNITS + 1, GU_UNITS, MLP_UNITS)),
        in_specs=[VMEM], out_specs=(VMEM,) * 3,
        scratch_shapes=[DMA((WINDOW // ATT_CHUNK + 1,)), DMA((4,)), DMA((WINDOW // MLP_CHUNK + 1,)), DMA((14,)), DMA((7,)), DMA, DMA],
        compiler_params=PARAMS,
    )(window)


def gather(gu_slabs, down_slabs, att_units):
    return pl.pallas_call(
        gather_kernel,
        out_shape=tuple(jax.ShapeDtypeStruct(shape, jnp.bfloat16) for shape in (
            (7 * CHIPS,) + gu_slabs.shape[1:], (7 * CHIPS,) + gu_slabs.shape[1:], (19 * DEVS,) + down_slabs.shape[1:],
            ((ATT_UNITS + 1) * DEVS, 8, 128))),
        in_specs=[VMEM] * 3, out_specs=(pl.BlockSpec(memory_space=pl.ANY),) * 4,
        scratch_shapes=[DMA((8, KINDS)), DMA((8, KINDS)), DMA((8, KINDS)), DMA((16, KINDS)), DMA((KINDS,)), DMA((CHIPS, KINDS)), DMA((CHIPS, KINDS))],
        compiler_params=PARAMS,
    )(gu_slabs, down_slabs, att_units)


def rope_tables(positions, head_dim):
    half_dim = head_dim // 2
    inv_freq = ROPE_BASE ** (-2.0 * jnp.arange(half_dim, dtype=jnp.float32) / head_dim)
    angles = positions.astype(jnp.float32)[:, :, None] * inv_freq
    cos_full = jnp.concatenate([jnp.cos(angles), jnp.cos(angles)], axis=-1)[:, :, None, :]
    sin_full = jnp.concatenate([jnp.sin(angles), jnp.sin(angles)], axis=-1)[:, :, None, :]
    return cos_full, sin_full


def rope_apply(values, cos_full, sin_full):
    half_dim = values.shape[-1] // 2
    rotated = jnp.concatenate([-values[..., half_dim:], values[..., :half_dim]], axis=-1)
    return values * cos_full + rotated * sin_full


def rope_back(grad_rot, cos_full, sin_full):
    half_dim = grad_rot.shape[-1] // 2
    scaled = grad_rot * sin_full
    return grad_rot * cos_full + jnp.concatenate([scaled[..., half_dim:], -scaled[..., :half_dim]], axis=-1)


def rms_parts(values):
    inv_rms = lax.rsqrt(jnp.mean(values * values, axis=-1, keepdims=True) + NORM_EPS)
    return inv_rms, values * inv_rms


def rms_back(d_normed, gain_wide, inv_rms, x_hat):
    d_hat = d_normed * gain_wide
    return inv_rms * (d_hat - x_hat * jnp.mean(d_hat * x_hat, axis=-1, keepdims=True))


def local_grads(x_loc, dy_loc, pos_loc, w_list, halos):
    attn_gain, w_query, w_key, w_value, w_out, mlp_gain, w_gate, w_up, w_down = w_list
    num_seqs, seq_len, model_dim = x_loc.shape
    num_heads, head_dim = w_query.shape[1], w_query.shape[2]
    kv_heads = w_key.shape[1]
    group_size = num_heads // kv_heads
    n_tok = num_seqs * seq_len
    wq_flat = w_query.reshape(model_dim, num_heads * head_dim)
    wk_flat = w_key.reshape(model_dim, kv_heads * head_dim)
    wv_flat = w_value.reshape(model_dim, kv_heads * head_dim)
    wo_flat = w_out.reshape(num_heads * head_dim, model_dim)
    dy_flat = dy_loc.reshape(n_tok, model_dim)
    x_wide = x_loc.reshape(n_tok, model_dim).astype(jnp.float32)
    inv_one, value_a8 = rms_parts(x_wide)
    gain_one = attn_gain.astype(jnp.float32)
    normed = (value_a8 * gain_one).astype(jnp.bfloat16)
    q_pre = jnp.dot(normed, wq_flat, preferred_element_type=jnp.float32).reshape(num_seqs, seq_len, num_heads, head_dim)
    k_pre = jnp.dot(normed, wk_flat, preferred_element_type=jnp.float32).reshape(num_seqs, seq_len, kv_heads, head_dim)
    v_heads = jnp.dot(normed, wv_flat, preferred_element_type=jnp.float32).astype(jnp.bfloat16).reshape(num_seqs, seq_len, kv_heads, head_dim)
    cos_full, sin_full = rope_tables(pos_loc, head_dim)
    q_rot = rope_apply(q_pre, cos_full, sin_full).astype(jnp.bfloat16).reshape(num_seqs, seq_len, kv_heads, group_size, head_dim)
    k_rot = rope_apply(k_pre, cos_full, sin_full).astype(jnp.bfloat16)
    score_scale = head_dim ** -0.5
    scores = jnp.einsum('bqkgd,bskd->bkgqs', q_rot, k_rot, preferred_element_type=jnp.float32) * score_scale
    causal = lax.iota(jnp.int32, seq_len)[:, None] >= lax.iota(jnp.int32, seq_len)[None, :]
    attn_probs = jax.nn.softmax(jnp.where(causal, scores, -1e30), axis=-1)
    probs_low = attn_probs.astype(jnp.bfloat16)
    context = jnp.einsum('bkgqs,bskd->bqkgd', probs_low, v_heads, preferred_element_type=jnp.float32).astype(jnp.bfloat16)
    context = context.reshape(n_tok, num_heads * head_dim)
    attn_out = jnp.dot(context, wo_flat, preferred_element_type=jnp.float32)
    hidden = (x_wide + attn_out).astype(jnp.bfloat16)
    inv_two, array_b8 = rms_parts(hidden.astype(jnp.float32))
    gain_two = mlp_gain.astype(jnp.float32)
    normed_mlp = (array_b8 * gain_two).astype(jnp.bfloat16)
    gate_pre = jnp.dot(normed_mlp, w_gate, preferred_element_type=jnp.float32)
    up_pre = jnp.dot(normed_mlp, w_up, preferred_element_type=jnp.float32)
    gate_sig = jax.nn.sigmoid(gate_pre)
    gate_act = gate_pre * gate_sig
    gated_act = (gate_act * up_pre).astype(jnp.bfloat16)
    g_down = jnp.einsum('nf,nd->fd', gated_act, dy_flat, preferred_element_type=jnp.float32)
    d_gated = jnp.einsum('nd,fd->nf', dy_flat, w_down, preferred_element_type=jnp.float32)
    d_up = (d_gated * gate_act).astype(jnp.bfloat16)
    d_gate = (d_gated * up_pre * gate_sig * (1.0 + gate_pre * (1.0 - gate_sig))).astype(jnp.bfloat16)
    g_gate = jnp.einsum('nd,nf->df', normed_mlp, d_gate, preferred_element_type=jnp.float32)
    g_up = jnp.einsum('nd,nf->df', normed_mlp, d_up, preferred_element_type=jnp.float32)
    mlp_units = (g_down.astype(jnp.bfloat16).reshape(-1, 8, model_dim), as_units(g_gate), as_units(g_up))
    down_shard, gate_shard = as_units(scatter(mlp_units[0])), scatter(mlp_units[1])
    _, d_gate, d_up, halos = lax.optimization_barrier((mlp_units, d_gate, d_up, halos))
    d_normed_mlp = (jnp.einsum('nf,df->nd', d_gate, w_gate, preferred_element_type=jnp.float32)
                    + jnp.einsum('nf,df->nd', d_up, w_up, preferred_element_type=jnp.float32))
    g_mlp_gain = jnp.sum(d_normed_mlp * array_b8, axis=0)
    d_hidden = rms_back(d_normed_mlp, gain_two, inv_two, array_b8) + dy_flat.astype(jnp.float32)
    d_hidden_low = d_hidden.astype(jnp.bfloat16)
    g_out = jnp.einsum('nc,nd->cd', context, d_hidden_low, preferred_element_type=jnp.float32)
    d_context = jnp.einsum('nd,cd->nc', d_hidden_low, wo_flat, preferred_element_type=jnp.float32).astype(jnp.bfloat16)
    d_context = d_context.reshape(num_seqs, seq_len, kv_heads, group_size, head_dim)
    d_probs = jnp.einsum('bqkgd,bskd->bkgqs', d_context, v_heads, preferred_element_type=jnp.float32)
    g_values = jnp.einsum('bkgqs,bqkgd->bskd', probs_low, d_context, preferred_element_type=jnp.float32)
    d_scores = (attn_probs * (d_probs - jnp.sum(d_probs * attn_probs, axis=-1, keepdims=True)) * score_scale).astype(jnp.bfloat16)
    d_q_rot = jnp.einsum('bkgqs,bskd->bqkgd', d_scores, k_rot, preferred_element_type=jnp.float32).reshape(num_seqs, seq_len, num_heads, head_dim)
    d_k_rot = jnp.einsum('bkgqs,bqkgd->bskd', d_scores, q_rot, preferred_element_type=jnp.float32)
    d_q_pre = rope_back(d_q_rot, cos_full, sin_full).astype(jnp.bfloat16).reshape(n_tok, num_heads * head_dim)
    d_k_pre = rope_back(d_k_rot, cos_full, sin_full).astype(jnp.bfloat16).reshape(n_tok, kv_heads * head_dim)
    d_v_pre = g_values.astype(jnp.bfloat16).reshape(n_tok, kv_heads * head_dim)
    g_query = jnp.einsum('nd,nc->dc', normed, d_q_pre, preferred_element_type=jnp.float32)
    g_key = jnp.einsum('nd,nc->dc', normed, d_k_pre, preferred_element_type=jnp.float32)
    g_value = jnp.einsum('nd,nc->dc', normed, d_v_pre, preferred_element_type=jnp.float32)
    d_normed = (jnp.einsum('nc,dc->nd', d_q_pre, wq_flat, preferred_element_type=jnp.float32)
                + jnp.einsum('nc,dc->nd', d_k_pre, wk_flat, preferred_element_type=jnp.float32)
                + jnp.einsum('nc,dc->nd', d_v_pre, wv_flat, preferred_element_type=jnp.float32))
    g_attn_gain = jnp.sum(d_normed * value_a8, axis=0)
    d_x = rms_back(d_normed, gain_one, inv_one, value_a8) + d_hidden
    pad_row = jnp.zeros((1, 128), jnp.bfloat16)
    gain_units = [jnp.concatenate([pad_row, g_gain.astype(jnp.bfloat16).reshape(-1, 128)]) for g_gain in (g_attn_gain, g_mlp_gain)]
    extra = jnp.concatenate([jnp.stack(gain_units), jnp.zeros((DEVS - 2, 8, 128), jnp.bfloat16)])
    att = jnp.concatenate([as_units(g) for g in (g_query, g_key, g_value, g_out)])
    att = jnp.concatenate([att.reshape(DEVS, ATT_UNITS, 8, 128), extra[:, None]], axis=1).reshape(-1, 8, 128)
    late = reduce_late(mlp_units[2], att)
    return d_x.astype(jnp.bfloat16).reshape(num_seqs, seq_len, model_dim), jnp.concatenate([late[MLP_UNITS:], gate_shard, late[:MLP_UNITS], down_shard]), halos
def adamw_apply(grad_vec, grad_norm, master_vec, mean_vec, var_vec, first_index, model_dim):
    clip_scale = jnp.minimum(1.0, 1.0 / (grad_norm + 1e-6))
    clipped = grad_vec * clip_scale
    new_mean = BETA_ONE * mean_vec + (1.0 - BETA_ONE) * clipped
    new_var = BETA_TWO * var_vec + (1.0 - BETA_TWO) * clipped * clipped
    mean_hat = new_mean / (1.0 - BETA_ONE ** STEP_COUNT)
    var_hat = new_var / (1.0 - BETA_TWO ** STEP_COUNT)
    flat_index = first_index + lax.iota(jnp.int32, master_vec.shape[0])
    is_gain = (flat_index < model_dim) | ((flat_index >= GAIN_TWO) & (flat_index < GAIN_TWO + model_dim))
    decays = jnp.where(is_gain, 0.0, WEIGHT_DECAY)
    new_master = master_vec - LEARN_RATE * (mean_hat / (jnp.sqrt(var_hat) + ADAM_EPS) + decays * master_vec)
    return new_master, new_mean, new_var


def solution(mesh):
    dp_size = mesh.shape['dp']
    ring_up = [(i, i + 1) for i in range(dp_size - 1)]

    def per_device(x_loc, dy_loc, pos_loc, attn_gain, w_query, w_key, w_value, w_out, mlp_gain, w_gate, w_up, w_down, master_loc, mean_loc, var_loc):
        w_list = (attn_gain, w_query, w_key, w_value, w_out, mlp_gain, w_gate, w_up, w_down)
        me = lax.axis_index('dp')
        state = (master_loc, mean_loc, var_loc)
        halo = lax.ppermute(jnp.stack([vec[BLOCK - HALO:] for vec in state]), 'dp', ring_up)
        grad_x, shard, halo = local_grads(x_loc, dy_loc, pos_loc, w_list, halo)
        part = jnp.sum(jnp.square(shard.astype(jnp.float32) / dp_size))
        part = jnp.where(lax.iota(jnp.int32, UNIT).reshape(1, 8, 128) == 0, part, 0.0)
        window, parts = spread(shard, part)
        grad_norm = jnp.sqrt(jnp.sum(parts))
        shift = (BLOCK * me + 128) % UNIT
        flat_win = window.reshape(-1)

        def update(first, length, vecs):
            index = BLOCK * me - HALO + first + lax.iota(jnp.int32, length)
            grads = jnp.where(index < GAIN_TWO, lax.dynamic_slice(flat_win, (shift + first,), (length,)),
                              lax.dynamic_slice(flat_win, (shift + first + 128,), (length,)))
            return adamw_apply(grads.astype(jnp.float32) / dp_size, grad_norm, vecs[0], vecs[1], vecs[2],
                               BLOCK * me - HALO + first, attn_gain.shape[0])
        new_state = update(HALO, BLOCK, state)
        low_main = new_state[0].astype(jnp.bfloat16)
        low_halo = update(0, HALO, halo)[0].astype(jnp.bfloat16)
        w_ext = jnp.pad(low_main, (LEAD + HALO, WINDOW * UNIT - BLOCK - HALO))
        w_ext = lax.dynamic_update_slice(w_ext, low_halo, (LEAD,))
        place = UNIT * (first_unit(me) - HALO_UNITS) + lax.iota(jnp.int32, WINDOW * UNIT)
        w_win = jnp.where(place < GAIN_UNIT * UNIT, lax.dynamic_slice(w_ext, (LEAD - shift,), (WINDOW * UNIT,)),
                          lax.dynamic_slice(w_ext, (LEAD - 128 - shift,), (WINDOW * UNIT,)))
        att_new, gu_new, down_new = collect(w_win.reshape(WINDOW, 8, 128))
        full = gather(gu_new.reshape(7, 8, w_gate.shape[1]), down_new.reshape(19, 8, w_down.shape[1]), att_new)
        full = (full[3],) + full[:3]
        att = full[0].reshape(DEVS, ATT_UNITS + 1, 8, 128)
        gains = [att[k, ATT_UNITS].reshape(-1)[128:] for k in range(2)]
        att = att[:, :ATT_UNITS].reshape(DEVS * ATT_UNITS, 8, 128)
        pieces = []
        offset = 0
        for weight in (w_query, w_key, w_value, w_out):
            pieces.append(att[offset:offset + weight.size // UNIT].reshape(weight.shape))
            offset += weight.size // UNIT
        new_weights = [gains[0]] + pieces + [gains[1], full[1].reshape(w_gate.shape), full[2].reshape(w_up.shape), full[3].reshape(w_down.shape)]
        return (grad_x,) + tuple(new_weights) + new_state + (grad_norm,)

    in_specs = (P('dp'),) * 3 + (P(),) * 9 + (P('dp'),) * 3
    out_specs = (P('dp'),) + (P(),) * 9 + (P('dp'),) * 3 + (P(),)
    return jax.shard_map(per_device, mesh=mesh, in_specs=in_specs, out_specs=out_specs, check_vma=False)
```

```python
import jax
import jax.numpy as jnp
from jax import lax
from jax.experimental import pallas as pl
from jax.experimental.pallas import tpu as pltpu
from jax.sharding import PartitionSpec as P

NORM_EPS = 1e-5
ROPE_BASE = 10000.0
LEARN_RATE = 2e-3
BETA_ONE = 0.9
BETA_TWO = 0.95
ADAM_EPS = 1e-8
WEIGHT_DECAY = 0.1
STEP_COUNT = 100


DEVS = 32
UNIT = 1024
BLOCK = 465976
ATT_UNITS = 56
MLP_UNITS = 133
GAIN_UNIT = 1 + DEVS * ATT_UNITS
MLP_UNIT = GAIN_UNIT + 1
GAIN_TWO = 1835904
ATT_CHUNK = 14
MLP_CHUNK = 19
GAIN_TWO = 1835904
GAIN_OWNER = GAIN_TWO // BLOCK
HALO_UNITS = 20
HALO = HALO_UNITS * UNIT
LEAD = 2048
CORE_UNITS = 457
WINDOW = HALO_UNITS + CORE_UNITS + MLP_CHUNK
SHARD = ATT_UNITS + 1 + 3 * MLP_UNITS
CHIPS = DEVS // 2
SLAB = 38
GU_UNITS = 7 * SLAB
PIECES = ((0, 1, ATT_UNITS, ATT_CHUNK), (ATT_UNITS + 1, MLP_UNIT, MLP_UNITS, MLP_CHUNK),
          (ATT_UNITS + 1 + MLP_UNITS, MLP_UNIT + DEVS * MLP_UNITS, MLP_UNITS, MLP_CHUNK),
          (ATT_UNITS + 1 + 2 * MLP_UNITS, MLP_UNIT + 2 * DEVS * MLP_UNITS, MLP_UNITS, MLP_CHUNK))


def as_units(grad):
    return grad.astype(jnp.bfloat16).reshape(-1, 8, 128)


def scatter(units):
    return lax.psum_scatter(units, 'dp', scatter_dimension=0, tiled=True)


def first_unit(owner):
    return (BLOCK * owner + 128) // UNIT


def last_owner(unit, chunk):
    return jnp.minimum((UNIT * (unit + chunk) - 129) // BLOCK, DEVS - 1)


def first_owner(unit):
    return (jnp.maximum(UNIT * (unit - CORE_UNITS + 1) - 128, 0) + BLOCK - 1) // BLOCK


def start_copy(source, target, peer, me, send_sem, recv_sem):
    @pl.when(peer == me)
    def _():
        pltpu.make_async_copy(source, target, recv_sem).start()

    @pl.when(peer != me)
    def _():
        pltpu.make_async_remote_copy(source, target, send_sem, recv_sem, device_id={'dp': peer}).start()


def end_send(source, target, peer, me, send_sem, recv_sem):
    @pl.when(peer != me)
    def _():
        pltpu.make_async_remote_copy(source, target, send_sem, recv_sem, device_id={'dp': peer}).wait_send()


def end_recv(target, recv_sem):
    pltpu.make_async_copy(target, target, recv_sem).wait()


def reach(unit, base, total, chunk):
    return jnp.minimum(jnp.maximum(unit - base, 0) // chunk, total)


def window_slot(unit, owner):
    return unit - first_unit(owner) + HALO_UNITS


def spread_kernel(shard_ref, part_ref, window_ref, parts_ref, att_send, att_recv, mlp_send, mlp_recv, part_send, part_recv, gain_send, gain_recv):
    me = lax.axis_index('dp')

    def place(unit, owner, size):
        return window_ref.at[pl.ds(window_slot(unit, owner), size)]

    def part_copy(step):
        return pltpu.make_async_remote_copy(part_ref, parts_ref.at[pl.ds(me, 1)], part_send.at[step], part_recv.at[me],
                                            device_id={'dp': lax.rem(me + step, DEVS)})

    def start_part(step, carry):
        part_copy(step).start()
        return carry

    def end_part(step, carry):
        part_copy(step).wait_send()
        return carry

    def take_part(peer, carry):
        end_recv(parts_ref.at[pl.ds(peer, 1)], part_recv.at[peer])
        return carry

    def each_chunk(action):
        first = 0
        for offset, base, count, chunk in PIECES:
            sends, recvs = (att_send, att_recv) if chunk == ATT_CHUNK else (mlp_send, mlp_recv)

            def step(index, carry, offset=offset, base=base, count=count, chunk=chunk, first=first, sends=sends, recvs=recvs):
                source = shard_ref.at[pl.ds(offset + index * chunk, chunk)]
                unit = base + me * count + index * chunk
                low, high = first_owner(unit), last_owner(unit, chunk)
                action(source, place(unit, high, chunk), high, me, sends.at[2 * (first + index)], recvs.at[window_slot(unit, high) // chunk])

                @pl.when(low != high)
                def _():
                    action(source, place(unit, low, chunk), low, me, sends.at[2 * (first + index) + 1],
                           recvs.at[window_slot(unit, low) // chunk])
                return carry
            lax.fori_loop(0, count // chunk, step, 0)
            first = 0 if chunk == ATT_CHUNK else first + count // chunk

    gain_source = shard_ref.at[pl.ds(ATT_UNITS, 1)]
    gain_two = pltpu.make_async_remote_copy(gain_source, place(GAIN_UNIT, GAIN_OWNER, 1), gain_send, gain_recv, device_id={'dp': GAIN_OWNER})
    gain_one = pltpu.make_async_copy(gain_source, place(0, 0, 1), gain_recv)
    pltpu.make_async_copy(part_ref, parts_ref.at[pl.ds(me, 1)], part_recv.at[me]).start()
    lax.fori_loop(1, DEVS, start_part, 0)

    @pl.when(me == 0)
    def _():
        gain_one.start()

    @pl.when(me == 1)
    def _():
        gain_two.start()

    each_chunk(start_copy)
    for base, total, chunk, recvs in ((1, DEVS * ATT_UNITS // ATT_CHUNK, ATT_CHUNK, att_recv),
                                      (MLP_UNIT, 3 * DEVS * MLP_UNITS // MLP_CHUNK, MLP_CHUNK, mlp_recv)):
        def take(index, carry, base=base, chunk=chunk, recvs=recvs):
            unit = base + index * chunk
            end_recv(place(unit, me, chunk), recvs.at[window_slot(unit, me) // chunk])
            return carry
        low = first_unit(me)
        lax.fori_loop(reach(low, base, total, chunk), reach(low + CORE_UNITS + chunk - 1, base, total, chunk), take, 0)
    each_chunk(end_send)
    lax.fori_loop(0, DEVS, take_part, 0)
    lax.fori_loop(1, DEVS, end_part, 0)

    @pl.when(me == 0)
    def _():
        gain_one.wait()

    @pl.when(me == 1)
    def _():
        gain_two.wait_send()

    @pl.when(me == GAIN_OWNER)
    def _():
        end_recv(place(GAIN_UNIT, me, 1), gain_recv)


def collect_kernel(window_ref, att_ref, gu_ref, down_ref, att_send, att_recv, mlp_send, gu_recv, down_recv, gain_send, gain_recv):
    me = lax.axis_index('dp')

    def slot(unit, size):
        return window_ref.at[pl.ds(window_slot(unit, me), size)]

    def even(index, per, target, recvs, chunk):
        peer = index // per
        within = index - peer * per
        return target.at[pl.ds(within * chunk, chunk)], peer, recvs.at[within]

    def slabs(index, cut):
        chip = index // 14
        half = index - chip * 14
        row = half // 2
        core = jnp.where(row >= cut, 1, 0)
        spot = jnp.where(row < 3, row, jnp.where(row == 3, 6, row - 4)) + jnp.where(row == 3, 0, 3 * (4 - cut))
        spot = 2 * spot + half - 2 * row
        return gu_ref.at[pl.ds(spot * MLP_CHUNK, MLP_CHUNK)], 2 * chip + core, gu_recv.at[spot]

    homes = (lambda index: even(index, 4, att_ref, att_recv, ATT_CHUNK), lambda index: slabs(index, 4),
             lambda index: slabs(index, 3), lambda index: even(index, 7, down_ref, down_recv, MLP_CHUNK))

    def each_chunk(action):
        for (_, base, count, chunk), home in zip(PIECES, homes):
            total = DEVS * count // chunk
            sends = att_send if chunk == ATT_CHUNK else mlp_send

            def step(index, carry, base=base, chunk=chunk, home=home, sends=sends):
                unit = base + index * chunk
                target, peer, recv = home(index)
                action(slot(unit, chunk), target, peer, me, sends.at[window_slot(unit, me) // chunk], recv)
                return carry
            high = jnp.where(me == DEVS - 1, total, reach(first_unit(me + 1), base, total, chunk))
            lax.fori_loop(reach(first_unit(me), base, total, chunk), high, step, 0)

    gain_target = att_ref.at[pl.ds(ATT_UNITS, 1)]
    gain_two = pltpu.make_async_remote_copy(slot(GAIN_UNIT, 1), gain_target, gain_send, gain_recv, device_id={'dp': 1})
    gain_one = pltpu.make_async_copy(slot(0, 1), gain_target, gain_recv)

    @pl.when(me == 0)
    def _():
        gain_one.start()

    @pl.when(me == GAIN_OWNER)
    def _():
        gain_two.start()

    each_chunk(start_copy)
    for target, recvs, chunk, count in ((att_ref, att_recv, ATT_CHUNK, 4), (gu_ref, gu_recv, MLP_CHUNK, 14), (down_ref, down_recv, MLP_CHUNK, 7)):
        def take(index, carry, target=target, recvs=recvs, chunk=chunk):
            end_recv(target.at[pl.ds(index * chunk, chunk)], recvs.at[index])
            return carry
        lax.fori_loop(0, count, take, 0)
    each_chunk(end_send)

    @pl.when(me == 0)
    def _():
        gain_one.wait()

    @pl.when(me == GAIN_OWNER)
    def _():
        gain_two.wait_send()

    @pl.when(me == 1)
    def _():
        end_recv(gain_target, gain_recv)


KINDS = 5


def gather_kernel(gu_in, down_in, att_in, gate_ref, up_ref, down_ref, att_ref, z_send, x_send, y_send, mate_send, home_sem, recv_sem, mate_sem):
    me = lax.axis_index('dp')
    core = lax.rem(me, 2)
    x = lax.rem(me // 2, 2)
    y = lax.rem(me // 4, 2)
    z = me // 8
    x_peer, y_peer, mate = me + 2 - 4 * x, me + 4 - 8 * y, me + 1 - 2 * core

    def blocks(chip, side, kind, own, action):
        def run(target, source):
            action(source if own else target, target)
        if kind == 0:
            run(gate_ref.at[pl.ds(7 * chip + 4 * side, 3)], gu_in.at[pl.ds(0, 3)])
        elif kind == 1:
            run(down_ref.at[pl.ds(19 * (2 * chip + side), 19)], down_in)
        elif kind == 2:
            run(up_ref.at[pl.ds(7 * chip + 4 * side, 3)], gu_in.at[pl.ds(3, 3)])
        elif kind == 3:
            run(att_ref.at[pl.ds((ATT_UNITS + 1) * (2 * chip + side), ATT_UNITS + 1)], att_in)
        else:
            @pl.when(side == 0)
            def _():
                run(gate_ref.at[pl.ds(7 * chip + 3, 1)], gu_in.at[pl.ds(6, 1)])

            @pl.when(side == 1)
            def _():
                run(up_ref.at[pl.ds(7 * chip + 3, 1)], gu_in.at[pl.ds(6, 1)])

    pushed = []

    def push(chip, kinds, peer, sends, recvs, own=False, when=None):
        def act(method):
            def body():
                for kind in kinds:
                    def action(source, target, kind=kind):
                        copy = pltpu.make_async_remote_copy(source, target, sends.at[kind], recvs.at[chip, kind], device_id={'dp': peer})
                        getattr(copy, method)()
                    blocks(chip, core, kind, own, action)
            if when is None:
                body()
            else:
                pl.when(when)(body)
        act('start')
        pushed.append(act)

    def take(chip, side, recvs, kinds=range(KINDS)):
        for kind in kinds:
            blocks(chip, side, kind, False, lambda source, target, kind=kind: end_recv(target, recvs.at[chip, kind]))

    def home(method):
        for kind in range(KINDS):
            blocks(me // 2, core, kind, True,
                   lambda source, target, kind=kind: getattr(pltpu.make_async_copy(source, target, home_sem.at[kind]), method)())

    every = tuple(range(KINDS))
    levels = (z, z + 1 - 2 * lax.rem(z, 2), jnp.where(z < 2, 2, 1), jnp.where(z < 2, 3, 0))

    def column(rank):
        level = levels[rank]
        chip = 4 * level + 2 * y + x
        own = rank == 0
        rise, sink = (z < 3, z > 0) if own else ((level < z) & (z < 3), (level > z) & (z > 0))
        for kind in every:
            if not own:
                take(chip, core, recv_sem, (kind,))
            push(chip, (kind,), me + 8, z_send.at[rank], recv_sem, own, rise)
            push(chip, (kind,), me - 8, z_send.at[4 + rank], recv_sem, own, sink)
            push(chip, (kind,), x_peer, x_send.at[rank], recv_sem, own)
            push(chip, (kind,), y_peer, y_send.at[rank], recv_sem, own)
            push(chip, (kind,), mate, mate_send.at[rank], mate_sem, own)

    def sides(rank):
        x_chip = 4 * levels[rank] + 2 * y + (1 - x)
        y_chip = 4 * levels[rank] + 2 * (1 - y) + x
        for kind in every:
            take(x_chip, core, recv_sem, (kind,))
            if kind >= 2:
                push(x_chip, (kind,), y_peer, y_send.at[4 + rank], recv_sem)
            push(x_chip, (kind,), mate, mate_send.at[4 + rank], mate_sem)
            take(y_chip, core, recv_sem, (kind,))
            if kind < 2:
                push(y_chip, (kind,), x_peer, x_send.at[4 + rank], recv_sem)
            push(y_chip, (kind,), mate, mate_send.at[8 + rank], mate_sem)

    def corner(rank):
        chip = 4 * levels[rank] + 2 * (1 - y) + (1 - x)
        for kind in every:
            take(chip, core, recv_sem, (kind,))
            push(chip, (kind,), mate, mate_send.at[12 + rank], mate_sem)

    home('start')
    for rank in range(6):
        if rank < 4:
            column(rank)
        if 1 <= rank < 5:
            sides(rank - 1)
        if rank >= 2:
            corner(rank - 2)
    home('wait')

    def take_mate(chip, carry):
        take(chip, 1 - core, mate_sem)
        return carry

    lax.fori_loop(0, CHIPS, take_mate, 0)
    for act in pushed:
        act('wait_send')


VMEM = pl.BlockSpec(memory_space=pltpu.VMEM)


LATE = MLP_UNITS + ATT_UNITS + 1
CUT = LATE // 2


def reduce_kernel(up_ref, extra_ref, query_ref, key_ref, value_ref, wout_ref, out_ref, pair, first, second, below, above, pair_send, pair_recv, a_send, a_recv, b_send, b_recv,
                  c_send, c_recv, d_send, d_recv, z_send, below_recv, above_recv):
    me = lax.axis_index('dp')
    core = lax.rem(me, 2)
    x = lax.rem(me // 2, 2)
    y = lax.rem(me // 4, 2)
    z = me // 8
    x_peer, y_peer, mate = me + 2 - 4 * x, me + 4 - 8 * y, me + 1 - 2 * core
    near = lax.rem(z, 2)
    levels = (jnp.where(z < 2, 3, 0), jnp.where(z < 2, 2, 1), z + 1 - 2 * near, z)
    halves = (pl.ds(0, CUT), pl.ds(CUT, CUT))

    def remote(source, target, send, recv, peer):
        return pltpu.make_async_remote_copy(source, target, send, recv, device_id={'dp': peer})

    def att_block(chip, side, action):
        @pl.when(chip < 7)
        def _():
            action(query_ref.at[chip, side])

        @pl.when(chip == 7)
        def _():
            action(key_ref.at[0, side])

        @pl.when(chip == 8)
        def _():
            action(value_ref.at[0, side])

        @pl.when(chip > 8)
        def _():
            action(wout_ref.at[chip - 9, side])

    def att_spot(level, number):
        return pair.at[level, number, pl.ds(MLP_UNITS, ATT_UNITS)]

    def att_copy(rank, number, source):
        return remote(source, att_spot(levels[rank], number), pair_send.at[rank, 2 + number], pair_recv.at[rank, 2 + number], mate)

    def pair_copies(rank):
        level = levels[rank]
        chips = pl.ds(4 * level, 4)
        return (remote(up_ref.at[chips, 1 - core], pair.at[level, :, pl.ds(0, MLP_UNITS)], pair_send.at[rank, 0], pair_recv.at[rank, 0], mate),
                remote(extra_ref.at[chips, 1 - core], pair.at[level, :, pl.ds(LATE - 1, 1)], pair_send.at[rank, 1], pair_recv.at[rank, 1], mate))

    def a_copies(rank):
        level = levels[rank]
        return [remote(pair.at[level, 2 * side + 1 - x, halves[0]], first.at[level, side, halves[0]], a_send.at[rank, side],
                       a_recv.at[rank, side], x_peer) for side in range(2)]

    def b_copies(rank):
        level = levels[rank]
        return [remote(pair.at[level, 2 * (1 - y) + side, halves[1]], first.at[level, side, halves[1]], b_send.at[rank, side],
                       b_recv.at[rank, side], y_peer) for side in range(2)]

    def c_copy(rank):
        level = levels[rank]
        return remote(first.at[level, 1 - y, halves[0]], second.at[level, halves[0]], c_send.at[rank], c_recv.at[rank], y_peer)

    def d_copy(rank):
        level = levels[rank]
        return remote(first.at[level, 1 - x, halves[1]], second.at[level, halves[1]], d_send.at[rank], d_recv.at[rank], x_peer)

    def up_copy(rank):
        level = levels[rank]
        return remote(second.at[level], below.at[level], z_send.at[rank], below_recv.at[level], me + 8)

    def down_copy(rank):
        level = levels[rank]
        return remote(second.at[level], above.at[level], z_send.at[rank], above_recv.at[level], me - 8)

    def add(target, source, count, step=19):
        def body(index, carry):
            rows = pl.ds(index * step, step)
            target[rows] = (target[rows].astype(jnp.float32) + source[rows].astype(jnp.float32)).astype(jnp.bfloat16)
            return carry
        lax.fori_loop(0, count // step, body, 0)

    def begin(rank):
        level = levels[rank]
        for copy in pair_copies(rank):
            copy.wait_recv()
        for chip in range(4):
            end_recv(att_spot(level, chip), pair_recv.at[rank, 2 + chip])
            add(pair.at[level, chip, pl.ds(0, MLP_UNITS)], up_ref.at[4 * level + chip, core], MLP_UNITS)
            add(pair.at[level, chip, pl.ds(LATE - 1, 1)], extra_ref.at[4 * level + chip, core], 1, 1)
            att_block(4 * level + chip, core, lambda ref, chip=chip: add(att_spot(level, chip), ref, ATT_UNITS, 14))
        for copy in a_copies(rank) + b_copies(rank):
            copy.start()

    def middle(rank):
        level = levels[rank]
        for copy in a_copies(rank) + b_copies(rank):
            copy.wait_recv()
        for side in range(2):
            add(first.at[level, side, halves[0]], pair.at[level, 2 * side + x, halves[0]], CUT)
            add(first.at[level, side, halves[1]], pair.at[level, 2 * y + side, halves[1]], CUT)
        c_copy(rank).start()
        d_copy(rank).start()

    def climb(rank):
        level = levels[rank]
        c_copy(rank).wait_recv()
        d_copy(rank).wait_recv()
        add(second.at[level, halves[0]], first.at[level, y, halves[0]], CUT)
        add(second.at[level, halves[1]], first.at[level, x, halves[1]], CUT)
        rising = (level >= z) & (z > 0)
        sinking = (level <= z) & (z < 3)

        @pl.when(rising)
        def _():
            pltpu.make_async_copy(below.at[level], below.at[level], below_recv.at[level]).wait()
            add(second.at[level], below.at[level], LATE)

        @pl.when(sinking)
        def _():
            pltpu.make_async_copy(above.at[level], above.at[level], above_recv.at[level]).wait()
            add(second.at[level], above.at[level], LATE)

        if rank < 3:
            @pl.when(level > z)
            def _():
                up_copy(rank).start()

            @pl.when(level < z)
            def _():
                down_copy(rank).start()
        else:
            def body(index, carry):
                rows = pl.ds(index * 19, 19)
                out_ref[rows] = second[level, rows]
                return carry
            lax.fori_loop(0, LATE // 19, body, 0)

    for rank in range(4):
        for copy in pair_copies(rank):
            copy.start()
        for number in range(4):
            att_block(4 * levels[rank] + number, 1 - core, lambda ref, rank=rank, number=number: att_copy(rank, number, ref).start())
    for step in range(6):
        if step < 4:
            begin(step)
        if 1 <= step < 5:
            middle(step - 1)
        if step >= 2:
            climb(step - 2)
    for rank in range(4):
        for copy in list(pair_copies(rank)) + a_copies(rank) + b_copies(rank) + [c_copy(rank), d_copy(rank)]:
            copy.wait_send()
        for number in range(4):
            att_copy(rank, number, query_ref.at[0, 0]).wait_send()
    for rank in range(3):
        @pl.when(levels[rank] > z)
        def _(rank=rank):
            up_copy(rank).wait_send()

        @pl.when(levels[rank] < z)
        def _(rank=rank):
            down_copy(rank).wait_send()


DMA = pltpu.SemaphoreType.DMA
PARAMS = pltpu.CompilerParams(has_side_effects=True)


def reduce_late(up_units, extra, att_units):
    shape = (8, 128)
    return pl.pallas_call(
        reduce_kernel,
        out_shape=jax.ShapeDtypeStruct((LATE,) + shape, jnp.bfloat16),
        in_specs=[VMEM] * 6, out_specs=VMEM,
        scratch_shapes=[pltpu.VMEM(dims + (LATE,) + shape, jnp.bfloat16) for dims in ((4, 4), (4, 2), (4,), (4,), (4,))]
        + [DMA((4, 6))] * 2 + [DMA((4, 2))] * 4 + [DMA((4,))] * 7,
        compiler_params=PARAMS,
    )(up_units.reshape((CHIPS, 2, MLP_UNITS) + shape), extra.reshape((CHIPS, 2, 1) + shape),
      *[units.reshape((-1, 2, ATT_UNITS) + shape) for units in att_units])


def spread(shard, part):
    return pl.pallas_call(
        spread_kernel,
        out_shape=(jax.ShapeDtypeStruct((WINDOW, 8, 128), jnp.bfloat16), jax.ShapeDtypeStruct((DEVS, 8, 128), jnp.float32)),
        in_specs=[VMEM] * 2, out_specs=(VMEM,) * 2,
        scratch_shapes=[DMA((8,)), DMA((WINDOW // ATT_CHUNK + 1,)), DMA((42,)), DMA((WINDOW // MLP_CHUNK + 1,)), DMA((DEVS,)), DMA((DEVS,)), DMA, DMA],
        compiler_params=PARAMS,
    )(shard, part)


def collect(window):
    return pl.pallas_call(
        collect_kernel,
        out_shape=tuple(jax.ShapeDtypeStruct((units, 8, 128), jnp.bfloat16) for units in (ATT_UNITS + 1, GU_UNITS, MLP_UNITS)),
        in_specs=[VMEM], out_specs=(VMEM,) * 3,
        scratch_shapes=[DMA((WINDOW // ATT_CHUNK + 1,)), DMA((4,)), DMA((WINDOW // MLP_CHUNK + 1,)), DMA((14,)), DMA((7,)), DMA, DMA],
        compiler_params=PARAMS,
    )(window)


def gather(gu_slabs, down_slabs, att_units):
    return pl.pallas_call(
        gather_kernel,
        out_shape=tuple(jax.ShapeDtypeStruct(shape, jnp.bfloat16) for shape in (
            (7 * CHIPS,) + gu_slabs.shape[1:], (7 * CHIPS,) + gu_slabs.shape[1:], (19 * DEVS,) + down_slabs.shape[1:],
            ((ATT_UNITS + 1) * DEVS, 8, 128))),
        in_specs=[VMEM] * 3, out_specs=(pl.BlockSpec(memory_space=pl.ANY),) * 4,
        scratch_shapes=[DMA((8, KINDS)), DMA((8, KINDS)), DMA((8, KINDS)), DMA((16, KINDS)), DMA((KINDS,)), DMA((CHIPS, KINDS)), DMA((CHIPS, KINDS))],
        compiler_params=PARAMS,
    )(gu_slabs, down_slabs, att_units)


def rope_tables(positions, head_dim):
    half_dim = head_dim // 2
    inv_freq = ROPE_BASE ** (-2.0 * jnp.arange(half_dim, dtype=jnp.float32) / head_dim)
    angles = positions.astype(jnp.float32)[:, :, None] * inv_freq
    cos_full = jnp.concatenate([jnp.cos(angles), jnp.cos(angles)], axis=-1)[:, :, None, :]
    sin_full = jnp.concatenate([jnp.sin(angles), jnp.sin(angles)], axis=-1)[:, :, None, :]
    return cos_full, sin_full


def rope_apply(values, cos_full, sin_full):
    half_dim = values.shape[-1] // 2
    rotated = jnp.concatenate([-values[..., half_dim:], values[..., :half_dim]], axis=-1)
    return values * cos_full + rotated * sin_full


def rope_back(grad_rot, cos_full, sin_full):
    half_dim = grad_rot.shape[-1] // 2
    scaled = grad_rot * sin_full
    return grad_rot * cos_full + jnp.concatenate([scaled[..., half_dim:], -scaled[..., :half_dim]], axis=-1)


def rms_parts(values):
    inv_rms = lax.rsqrt(jnp.mean(values * values, axis=-1, keepdims=True) + NORM_EPS)
    return inv_rms, values * inv_rms


def rms_back(d_normed, gain_wide, inv_rms, x_hat):
    d_hat = d_normed * gain_wide
    return inv_rms * (d_hat - x_hat * jnp.mean(d_hat * x_hat, axis=-1, keepdims=True))


def local_grads(x_loc, dy_loc, pos_loc, w_list, halos):
    attn_gain, w_query, w_key, w_value, w_out, mlp_gain, w_gate, w_up, w_down = w_list
    num_seqs, seq_len, model_dim = x_loc.shape
    num_heads, head_dim = w_query.shape[1], w_query.shape[2]
    kv_heads = w_key.shape[1]
    group_size = num_heads // kv_heads
    n_tok = num_seqs * seq_len
    wq_flat = w_query.reshape(model_dim, num_heads * head_dim)
    wk_flat = w_key.reshape(model_dim, kv_heads * head_dim)
    wv_flat = w_value.reshape(model_dim, kv_heads * head_dim)
    wo_flat = w_out.reshape(num_heads * head_dim, model_dim)
    dy_flat = dy_loc.reshape(n_tok, model_dim)
    x_wide = x_loc.reshape(n_tok, model_dim).astype(jnp.float32)
    inv_one, value_a8 = rms_parts(x_wide)
    gain_one = attn_gain.astype(jnp.float32)
    normed = (value_a8 * gain_one).astype(jnp.bfloat16)
    q_pre = jnp.dot(normed, wq_flat, preferred_element_type=jnp.float32).reshape(num_seqs, seq_len, num_heads, head_dim)
    k_pre = jnp.dot(normed, wk_flat, preferred_element_type=jnp.float32).reshape(num_seqs, seq_len, kv_heads, head_dim)
    v_heads = jnp.dot(normed, wv_flat, preferred_element_type=jnp.float32).astype(jnp.bfloat16).reshape(num_seqs, seq_len, kv_heads, head_dim)
    cos_full, sin_full = rope_tables(pos_loc, head_dim)
    q_rot = rope_apply(q_pre, cos_full, sin_full).astype(jnp.bfloat16).reshape(num_seqs, seq_len, kv_heads, group_size, head_dim)
    k_rot = rope_apply(k_pre, cos_full, sin_full).astype(jnp.bfloat16)
    score_scale = head_dim ** -0.5
    scores = jnp.einsum('bqkgd,bskd->bkgqs', q_rot, k_rot, preferred_element_type=jnp.float32) * score_scale
    causal = lax.iota(jnp.int32, seq_len)[:, None] >= lax.iota(jnp.int32, seq_len)[None, :]
    attn_probs = jax.nn.softmax(jnp.where(causal, scores, -1e30), axis=-1)
    probs_low = attn_probs.astype(jnp.bfloat16)
    context = jnp.einsum('bkgqs,bskd->bqkgd', probs_low, v_heads, preferred_element_type=jnp.float32).astype(jnp.bfloat16)
    context = context.reshape(n_tok, num_heads * head_dim)
    attn_out = jnp.dot(context, wo_flat, preferred_element_type=jnp.float32)
    hidden = (x_wide + attn_out).astype(jnp.bfloat16)
    inv_two, array_b8 = rms_parts(hidden.astype(jnp.float32))
    gain_two = mlp_gain.astype(jnp.float32)
    normed_mlp = (array_b8 * gain_two).astype(jnp.bfloat16)
    gate_pre = jnp.dot(normed_mlp, w_gate, preferred_element_type=jnp.float32)
    up_pre = jnp.dot(normed_mlp, w_up, preferred_element_type=jnp.float32)
    gate_sig = jax.nn.sigmoid(gate_pre)
    gate_act = gate_pre * gate_sig
    gated_act = (gate_act * up_pre).astype(jnp.bfloat16)
    g_down = jnp.einsum('nf,nd->fd', gated_act, dy_flat, preferred_element_type=jnp.float32)
    d_gated = jnp.einsum('nd,fd->nf', dy_flat, w_down, preferred_element_type=jnp.float32)
    d_up = (d_gated * gate_act).astype(jnp.bfloat16)
    d_gate = (d_gated * up_pre * gate_sig * (1.0 + gate_pre * (1.0 - gate_sig))).astype(jnp.bfloat16)
    g_gate = jnp.einsum('nd,nf->df', normed_mlp, d_gate, preferred_element_type=jnp.float32)
    g_up = jnp.einsum('nd,nf->df', normed_mlp, d_up, preferred_element_type=jnp.float32)
    mlp_units = (g_down.astype(jnp.bfloat16).reshape(-1, 8, model_dim), as_units(g_gate), as_units(g_up))
    down_shard, gate_shard = as_units(scatter(mlp_units[0])), scatter(mlp_units[1])
    _, d_gate, d_up, halos = lax.optimization_barrier((mlp_units, d_gate, d_up, halos))
    d_normed_mlp = (jnp.einsum('nf,df->nd', d_gate, w_gate, preferred_element_type=jnp.float32)
                    + jnp.einsum('nf,df->nd', d_up, w_up, preferred_element_type=jnp.float32))
    g_mlp_gain = jnp.sum(d_normed_mlp * array_b8, axis=0)
    d_hidden = rms_back(d_normed_mlp, gain_two, inv_two, array_b8) + dy_flat.astype(jnp.float32)
    d_hidden_low = d_hidden.astype(jnp.bfloat16)
    g_out = jnp.einsum('nc,nd->cd', context, d_hidden_low, preferred_element_type=jnp.float32)
    d_context = jnp.einsum('nd,cd->nc', d_hidden_low, wo_flat, preferred_element_type=jnp.float32).astype(jnp.bfloat16)
    d_context = d_context.reshape(num_seqs, seq_len, kv_heads, group_size, head_dim)
    d_probs = jnp.einsum('bqkgd,bskd->bkgqs', d_context, v_heads, preferred_element_type=jnp.float32)
    g_values = jnp.einsum('bkgqs,bqkgd->bskd', probs_low, d_context, preferred_element_type=jnp.float32)
    d_scores = (attn_probs * (d_probs - jnp.sum(d_probs * attn_probs, axis=-1, keepdims=True)) * score_scale).astype(jnp.bfloat16)
    d_q_rot = jnp.einsum('bkgqs,bskd->bqkgd', d_scores, k_rot, preferred_element_type=jnp.float32).reshape(num_seqs, seq_len, num_heads, head_dim)
    d_k_rot = jnp.einsum('bkgqs,bqkgd->bskd', d_scores, q_rot, preferred_element_type=jnp.float32)
    d_q_pre = rope_back(d_q_rot, cos_full, sin_full).astype(jnp.bfloat16).reshape(n_tok, num_heads * head_dim)
    d_k_pre = rope_back(d_k_rot, cos_full, sin_full).astype(jnp.bfloat16).reshape(n_tok, kv_heads * head_dim)
    d_v_pre = g_values.astype(jnp.bfloat16).reshape(n_tok, kv_heads * head_dim)
    g_query = jnp.einsum('nd,nc->dc', normed, d_q_pre, preferred_element_type=jnp.float32)
    g_key = jnp.einsum('nd,nc->dc', normed, d_k_pre, preferred_element_type=jnp.float32)
    g_value = jnp.einsum('nd,nc->dc', normed, d_v_pre, preferred_element_type=jnp.float32)
    d_normed = (jnp.einsum('nc,dc->nd', d_q_pre, wq_flat, preferred_element_type=jnp.float32)
                + jnp.einsum('nc,dc->nd', d_k_pre, wk_flat, preferred_element_type=jnp.float32)
                + jnp.einsum('nc,dc->nd', d_v_pre, wv_flat, preferred_element_type=jnp.float32))
    g_attn_gain = jnp.sum(d_normed * value_a8, axis=0)
    d_x = rms_back(d_normed, gain_one, inv_one, value_a8) + d_hidden
    pad_row = jnp.zeros((1, 128), jnp.bfloat16)
    gain_units = [jnp.concatenate([pad_row, g_gain.astype(jnp.bfloat16).reshape(-1, 128)]) for g_gain in (g_attn_gain, g_mlp_gain)]
    extra = jnp.concatenate([jnp.stack(gain_units), jnp.zeros((DEVS - 2, 8, 128), jnp.bfloat16)])
    late = reduce_late(mlp_units[2], extra, [as_units(g) for g in (g_query, g_key, g_value, g_out)])
    return d_x.astype(jnp.bfloat16).reshape(num_seqs, seq_len, model_dim), jnp.concatenate([late[MLP_UNITS:], gate_shard, late[:MLP_UNITS], down_shard]), halos
def adamw_apply(grad_vec, grad_norm, master_vec, mean_vec, var_vec, first_index, model_dim):
    clip_scale = jnp.minimum(1.0, 1.0 / (grad_norm + 1e-6))
    clipped = grad_vec * clip_scale
    new_mean = BETA_ONE * mean_vec + (1.0 - BETA_ONE) * clipped
    new_var = BETA_TWO * var_vec + (1.0 - BETA_TWO) * clipped * clipped
    mean_hat = new_mean / (1.0 - BETA_ONE ** STEP_COUNT)
    var_hat = new_var / (1.0 - BETA_TWO ** STEP_COUNT)
    flat_index = first_index + lax.iota(jnp.int32, master_vec.shape[0])
    is_gain = (flat_index < model_dim) | ((flat_index >= GAIN_TWO) & (flat_index < GAIN_TWO + model_dim))
    decays = jnp.where(is_gain, 0.0, WEIGHT_DECAY)
    new_master = master_vec - LEARN_RATE * (mean_hat / (jnp.sqrt(var_hat) + ADAM_EPS) + decays * master_vec)
    return new_master, new_mean, new_var


def solution(mesh):
    dp_size = mesh.shape['dp']
    ring_up = [(i, i + 1) for i in range(dp_size - 1)]

    def per_device(x_loc, dy_loc, pos_loc, attn_gain, w_query, w_key, w_value, w_out, mlp_gain, w_gate, w_up, w_down, master_loc, mean_loc, var_loc):
        w_list = (attn_gain, w_query, w_key, w_value, w_out, mlp_gain, w_gate, w_up, w_down)
        me = lax.axis_index('dp')
        state = (master_loc, mean_loc, var_loc)
        halo = lax.ppermute(jnp.stack([vec[BLOCK - HALO:] for vec in state]), 'dp', ring_up)
        grad_x, shard, halo = local_grads(x_loc, dy_loc, pos_loc, w_list, halo)
        part = jnp.sum(jnp.square(shard.astype(jnp.float32) / dp_size))
        part = jnp.where(lax.iota(jnp.int32, UNIT).reshape(1, 8, 128) == 0, part, 0.0)
        window, parts = spread(shard, part)
        grad_norm = jnp.sqrt(jnp.sum(parts))
        shift = (BLOCK * me + 128) % UNIT
        flat_win = window.reshape(-1)

        def update(first, length, vecs):
            index = BLOCK * me - HALO + first + lax.iota(jnp.int32, length)
            grads = jnp.where(index < GAIN_TWO, lax.dynamic_slice(flat_win, (shift + first,), (length,)),
                              lax.dynamic_slice(flat_win, (shift + first + 128,), (length,)))
            return adamw_apply(grads.astype(jnp.float32) / dp_size, grad_norm, vecs[0], vecs[1], vecs[2],
                               BLOCK * me - HALO + first, attn_gain.shape[0])
        new_state = update(HALO, BLOCK, state)
        low_main = new_state[0].astype(jnp.bfloat16)
        low_halo = update(0, HALO, halo)[0].astype(jnp.bfloat16)
        w_ext = jnp.pad(low_main, (LEAD + HALO, WINDOW * UNIT - BLOCK - HALO))
        w_ext = lax.dynamic_update_slice(w_ext, low_halo, (LEAD,))
        place = UNIT * (first_unit(me) - HALO_UNITS) + lax.iota(jnp.int32, WINDOW * UNIT)
        w_win = jnp.where(place < GAIN_UNIT * UNIT, lax.dynamic_slice(w_ext, (LEAD - shift,), (WINDOW * UNIT,)),
                          lax.dynamic_slice(w_ext, (LEAD - 128 - shift,), (WINDOW * UNIT,)))
        att_new, gu_new, down_new = collect(w_win.reshape(WINDOW, 8, 128))
        full = gather(gu_new.reshape(7, 8, w_gate.shape[1]), down_new.reshape(19, 8, w_down.shape[1]), att_new)
        full = (full[3],) + full[:3]
        att = full[0].reshape(DEVS, ATT_UNITS + 1, 8, 128)
        gains = [att[k, ATT_UNITS].reshape(-1)[128:] for k in range(2)]
        att = att[:, :ATT_UNITS].reshape(DEVS * ATT_UNITS, 8, 128)
        pieces = []
        offset = 0
        for weight in (w_query, w_key, w_value, w_out):
            pieces.append(att[offset:offset + weight.size // UNIT].reshape(weight.shape))
            offset += weight.size // UNIT
        new_weights = [gains[0]] + pieces + [gains[1], full[1].reshape(w_gate.shape), full[2].reshape(w_up.shape), full[3].reshape(w_down.shape)]
        return (grad_x,) + tuple(new_weights) + new_state + (grad_norm,)

    in_specs = (P('dp'),) * 3 + (P(),) * 9 + (P('dp'),) * 3
    out_specs = (P('dp'),) + (P(),) * 9 + (P('dp'),) * 3 + (P(),)
    return jax.shard_map(per_device, mesh=mesh, in_specs=in_specs, out_specs=out_specs, check_vma=False)
```
